256 devices in a mesh: gx: 4 (over z_hi), gy: 8 (over x, core), gz: 8 (over y, z_lo).
Axes of the slice: x: 4, y: 4, z: 8 (z_hi: 4, z_lo: 2; z = z_hi * 2 + z_lo), core: 2. Of those that a mesh axis runs over, the one named last changes fastest.
Arguments:
- order_real: float32 [128, 256, 1024], P('gz', 'gx', 'gy'), may hold values from -2.5 to 2.5
- order_imag: float32 [128, 256, 1024], P('gz', 'gx', 'gy'), may hold values from -2.5 to 2.5
- phase_z: float32 [128, 256, 1024], P('gz', 'gx', 'gy'), may hold values from -3.140625 to 3.140625
- phase_x: float32 [128, 256, 1024], P('gz', 'gx', 'gy'), may hold values from -3.140625 to 3.140625
- phase_y: float32 [128, 256, 1024], P('gz', 'gx', 'gy'), may hold values from -3.140625 to 3.140625
- material: int32 [128, 256, 1024], P('gz', 'gx', 'gy'), may hold values from 0 to 7
- levels: float32 [8], replicated, may hold values from -0.5 to 1.5
Outputs:
- final_real: float32 [128, 256, 1024], P('gz', 'gx', 'gy')
- final_imag: float32 [128, 256, 1024], P('gz', 'gx', 'gy')
- circulation: float32 [128, 256, 1024], P('gz', ('gx', 'gy'))
- current_flux: float32 [128, 256, 1024], P('gz', ('gx', 'gy'))
The draws below stay inside these ranges and needn't reach their ends.
All inputs are finite; a program needn't handle non-finite values.
Results may differ from the reference program's by a relative error of at most 0.0003.
Values sent between devices are 32-bit elements; how exact they have to be, the bound alone decides.
No kernel may reach another device: no remote copies, remote signals or barrier semaphores. Data moves between devices by JAX's collectives and lax.ppermute only.
A program may use at most 64 MiB of HBM per device.

```python
import jax
import jax.numpy as jnp

STEPS = 2
LEVELS = 8
NZ = 128
NX = 256
NY = 1024


def place_ends(array, rng, least, top_value):
    longest = array.shape.index(max(array.shape))
    spots = []
    for shift in (0, 1):
        where = [jax.random.randint(jax.random.fold_in(rng, axis), (), 0, length) for axis, length in enumerate(array.shape)]
        where[longest] = (where[longest] + shift) % array.shape[longest]
        spots.append(tuple(where))
    return array.at[spots[0]].set(least).at[spots[1]].set(top_value)


def block_levels(own_key, extent, pieces, smallest, high):
    def one(position, shards_of):
        steps = jax.random.uniform(jax.random.fold_in(jax.random.fold_in(own_key, 6), position), (shards_of,), jnp.float32, smallest / len(pieces), high / len(pieces))
        return jnp.repeat(jnp.exp(steps), extent[position] // shards_of).reshape((-1,) + (1,) * (len(extent) - position - 1))

    loudness = one(*pieces[0])
    for cut in pieces[1:]:
        loudness = loudness * one(*cut)
    return loudness


def gaussian(stream_key, dims, deviation, reach, split=(), dtype=jnp.bfloat16):
    values = deviation * jax.random.normal(stream_key, dims, jnp.float32)
    if split:
        values = values * block_levels(stream_key, dims, split, -0.22, 0.18)
    return jnp.clip(values, -reach, reach).astype(dtype)


def setup_inputs(seed: int = 0) -> dict:
    arg_keys = jax.random.split(jax.random.key(seed), 8)
    order_real = gaussian(arg_keys[0], (NZ, NX, NY), 0.6, 2.5, ((0, 8), (1, 4), (2, 8)), jnp.float32)
    order_imag = gaussian(arg_keys[1], (NZ, NX, NY), 0.6, 2.5, ((0, 8), (1, 4), (2, 8)), jnp.float32)
    phase_z = jnp.clip(jax.random.uniform(arg_keys[2], (NZ, NX, NY), jnp.float32, -3.140625, 3.140625), -3.140625, 3.140625)
    phase_x = jnp.clip(jax.random.uniform(arg_keys[3], (NZ, NX, NY), jnp.float32, -3.140625, 3.140625), -3.140625, 3.140625)
    phase_y = jnp.clip(jax.random.uniform(arg_keys[4], (NZ, NX, NY), jnp.float32, -3.140625, 3.140625), -3.140625, 3.140625)
    material = place_ends(jax.random.randint(arg_keys[5], (NZ, NX, NY), 0, LEVELS), jax.random.fold_in(arg_keys[5], 1), 0, LEVELS - 1).astype(jnp.int32)
    levels = jnp.clip(jax.random.uniform(arg_keys[6], (LEVELS,), jnp.float32, -0.5, 1.5), -0.5, 1.5)
    return dict(order_real=order_real, order_imag=order_imag, phase_z=phase_z, phase_x=phase_x, phase_y=phase_y, material=material, levels=levels)


time_step = 0.15


def inner(values, direction, offset):
    slicer = [slice(1, length - 1) for length in values.shape]
    length = values.shape[direction]
    slicer[direction] = slice(1 + offset, length - 1 + offset)
    return values[tuple(slicer)]


def advance(real_part, imag_part, cosines, sine_parts, epsilon, inside_mask):
    centre_real = inner(real_part, 0, 0)
    centre_imag = inner(imag_part, 0, 0)
    lap_real = -6.0 * centre_real
    lap_imag = -6.0 * centre_imag
    for direction in range(3):
        cosine = inner(cosines[direction], direction, 0)
        sine_part = inner(sine_parts[direction], direction, 0)
        ahead_real = inner(real_part, direction, 1)
        ahead_imag = inner(imag_part, direction, 1)
        lap_real = lap_real + cosine * ahead_real - sine_part * ahead_imag
        lap_imag = lap_imag + cosine * ahead_imag + sine_part * ahead_real
        cosine = inner(cosines[direction], direction, -1)
        sine_part = inner(sine_parts[direction], direction, -1)
        behind_real = inner(real_part, direction, -1)
        behind_imag = inner(imag_part, direction, -1)
        lap_real = lap_real + cosine * behind_real + sine_part * behind_imag
        lap_imag = lap_imag + cosine * behind_imag - sine_part * behind_real
    density = centre_real * centre_real + centre_imag * centre_imag
    new_real = centre_real + time_step * ((epsilon - density) * centre_real + lap_real)
    new_imag = centre_imag + time_step * ((epsilon - density) * centre_imag + lap_imag)
    if inside_mask is not None:
        new_real = new_real * inside_mask
        new_imag = new_imag * inside_mask
    return new_real, new_imag


def current(first_real, first_imag, second_real, second_imag, phase):
    cosine = jnp.cos(phase)
    sine_part = jnp.sin(phase)
    turned_real = cosine * second_real - sine_part * second_imag
    turned_imag = cosine * second_imag + sine_part * second_real
    return first_real * turned_imag - first_imag * turned_real


def analyse(upper_real, upper_imag, phase_along_x, phase_along_y):
    rows = phase_along_x.shape[1]
    cols = phase_along_y.shape[2]
    current_x = current(upper_real[:, :rows, :], upper_imag[:, :rows, :], upper_real[:, 1:, :], upper_imag[:, 1:, :], phase_along_x)
    current_y = current(upper_real[:, :, :cols], upper_imag[:, :, :cols], upper_real[:, :, 1:], upper_imag[:, :, 1:], phase_along_y)
    circulation = current_x[:, :, :cols] + current_y[:, 1:, :] - current_x[:, :, 1:] - current_y[:, :rows, :]
    return circulation, current_x[:, :, :cols]


def reference(order_real, order_imag, phase_z, phase_x, phase_y, material, levels):
    epsilon = levels[material]
    padded = [jnp.pad(phase, 1) for phase in (phase_z, phase_x, phase_y)]
    cosines = [jnp.cos(phase) for phase in padded]
    sine_parts = [jnp.sin(phase) for phase in padded]
    real_part, imag_part = order_real, order_imag
    for turn in range(STEPS):
        real_part, imag_part = advance(jnp.pad(real_part, 1), jnp.pad(imag_part, 1), cosines, sine_parts, epsilon, None)
    upper = ((0, 0), (0, 1), (0, 1))
    circulation, current_x = analyse(jnp.pad(real_part, upper), jnp.pad(imag_part, upper),
                                     jnp.pad(phase_x, ((0, 0), (0, 0), (0, 1))), jnp.pad(phase_y, ((0, 0), (0, 1), (0, 0))))
    current_flux = jnp.cumsum(current_x, axis=2)
    return real_part, imag_part, circulation, current_flux
```

```python
import functools

import jax
import jax.numpy as jnp
from jax import lax
from jax.experimental import pallas as pl
from jax.experimental.pallas import tpu as pltpu
from jax.sharding import PartitionSpec as P

LEVELS = 8
time_step = 0.15

F32 = jnp.float32
LANES = 128
TILE = 8
NZ, NX, NY = 16, 64, 128
RX = NX + TILE
PR, PI, PX, PY, PZ, EP = range(6)

SIN = (1.0, -0.16666658222675323, 0.008333050645887852, -0.00019809069635812193, 2.6052216526295524e-06)
COS = (-0.5, 0.0416666604578495, -0.0013888651737943292, 2.4774621124379337e-05, -2.6298400257473986e-07)


def sincos(phase):
    half = phase * 0.5
    u = half * half
    s = SIN[4]
    for k in (3, 2, 1, 0):
        s = s * u + SIN[k]
    s = s * half
    c = COS[4]
    for k in (3, 2, 1, 0):
        c = c * u + COS[k]
    c = c * u + 1.0
    return (c - s) * (c + s), (s + s) * c


def iota(shape, dim):
    return lax.broadcasted_iota(jnp.int32, shape, dim)


def roll(v, shift, axis):
    return pltpu.roll(v, shift % v.shape[axis], axis)


def ahead_x(v):
    return pltpu.roll(v, RX - 1, 0)


def behind_x(v):
    return pltpu.roll(v, 1, 0)


def turned(c, s, r, i):
    return c * r - s * i, c * i + s * r


def turned_back(c, s, r, i):
    return c * r + s * i, c * i - s * r


def choose(index, cases):
    out = cases[-1][1]
    for test, value in cases[-2::-1]:
        out = jnp.where(test(index), value, out)
    return out


def place_low(index, r, i, c, s, others, own):
    wr, wi = turned_back(c, s, r, i)
    first = index == own
    return jnp.where(first, wr, r), jnp.where(first, wi, i)


def row_up(a, row):
    pr, pi, px, py, pz, ep = a
    c, s = sincos(px)
    wr, wi = turned_back(c, s, pr, pi)
    last = row == 6
    pr = jnp.where(last, wr, pr)
    pi = jnp.where(last, wi, pi)
    out = roll(pr, 2, 0)
    out = jnp.where(row >= 2, roll(pi, 4, 0), out)
    out = jnp.where(row == 4, roll(px, 5, 0), out)
    out = jnp.where(row == 5, roll(py, 6, 0), out)
    out = jnp.where(row == 6, roll(pz, 7, 0), out)
    return jnp.where(row == 7, ep, out)


def row_down(a, row):
    pr, pi, px, py, pz, ep = a
    first = jnp.where(row < 3, pr, jnp.where(row < 6, roll(pi, 3, 0), roll(px, 6, 0)))
    second = jnp.where(row < 2, py, jnp.where(row < 4, roll(pz, 2, 0), roll(ep, 4, 0)))
    return first, second


def pack_x(levels, pr, pi, px, py, pz, mat, ep, up, down):
    row = iota((TILE, LANES), 0)

    def body(z, carry):
        m = mat[z]
        e = jnp.full((NX, NY), levels[LEVELS - 1], F32)
        for k in range(LEVELS - 1):
            e = jnp.where(m == k, levels[k], e)
        ep[z] = e
        top = [q[z, NX - TILE:, :] for q in (pr, pi, px, py, pz)] + [e[NX - TILE:, :]]
        low = [q[z, :TILE, :] for q in (pr, pi, px, py, pz)] + [e[:TILE, :]]
        up[z] = row_up(top, row)
        first, second = row_down(low, row)
        down[z, :TILE, :] = first
        down[z, TILE:, :] = second
        return carry

    lax.fori_loop(0, NZ, body, 0)


def pack_y(pr, pi, px, py, pz, ep, lo, hi, halo, own, up, down):
    row = iota((TILE, LANES), 0)
    gx = lax.axis_index("gx")
    keep = jnp.where(row < 4, jnp.where(gx < lax.axis_size("gx") - 1, 1, 0), jnp.where(gx > 0, 1, 0)) > 0
    low_rows = row >= 6

    def unpack(z, carry):
        l = lo[z]
        a = hi[z, :TILE, :]
        b = hi[z, TILE:, :]
        zero = jnp.zeros_like(l)
        last = row == 7
        halo[PR, z] = jnp.where(keep, jnp.where(low_rows, roll(l, 6, 0), a), zero)
        halo[PI, z] = jnp.where(keep, jnp.where(low_rows, roll(l, 4, 0), roll(a, -3, 0)), zero)
        halo[PX, z] = jnp.where(last, roll(l, 3, 0), jnp.where(row < 2, roll(a, -6, 0), zero))
        halo[PY, z] = jnp.where(last, roll(l, 2, 0), jnp.where(row < 2, b, zero))
        halo[PZ, z] = jnp.where(last, roll(l, 1, 0), jnp.where(row < 2, roll(b, -2, 0), zero))
        halo[EP, z] = jnp.where(last, l, jnp.where(row < 2, roll(b, -4, 0), zero))
        return carry

    lax.fori_loop(0, NZ, unpack, 0)
    lane = iota((RX, LANES), 1)
    slot = lane % 8
    group = lane // 8
    columns = []
    for k, q in enumerate((pr, pi, px, py, pz, ep)):
        acc = jnp.zeros((RX, LANES), F32)
        for z in range(NZ):
            v = jnp.concatenate([q[z], halo[k, z]], axis=0)
            acc = jnp.where(group == z, roll(v, 8 * z - 126, 1), acc)
        own[k] = acc
        columns.append(acc)
    vr, vi, vx, vy, vz, ve = columns
    c, s = sincos(vy)
    wr, wi = turned_back(c, s, vr, vi)
    ur = jnp.where(slot == 0, wr, vr)
    ui = jnp.where(slot == 0, wi, vi)
    out = jnp.where(slot < 2, ur, roll(ui, 2, 1))
    out = jnp.where(slot == 4, roll(vx, 3, 1), out)
    out = jnp.where(slot == 5, roll(vy, 4, 1), out)
    out = jnp.where(slot == 6, roll(vz, 5, 1), out)
    out = jnp.where(slot == 7, roll(ve, 6, 1), out)
    up[...] = out
    down[0] = jnp.where(slot < 3, roll(vr, -2, 1), jnp.where(slot < 6, roll(vi, 1, 1), roll(vx, 4, 1)))
    down[1] = jnp.where(slot < 2, roll(vy, -2, 1), jnp.where(slot < 4, vz, roll(ve, 2, 1)))


def pack_z(pr, pi, px, py, pz, ep, halo, own, lo, hi, strip, up, down):
    lane = iota((RX, LANES), 1)
    slot = lane % 8
    group = lane // 8
    gy = lax.axis_index("gy")
    keep = jnp.where((slot >= 2) & (slot < 5), jnp.where(gy < lax.axis_size("gy") - 1, 1, 0),
                     jnp.where((slot >= 5) & (slot < 7), jnp.where(gy > 0, 1, 0), 1)) > 0
    l = lo[...]
    a = hi[0]
    b = hi[1]
    zero = jnp.zeros_like(l)

    def join(k, from_hi, from_lo):
        v = own[k]
        out = jnp.where(slot < 2, v, roll(v, 5, 1))
        out = jnp.where((slot >= 2) & (slot < 5), from_hi, out)
        return jnp.where((slot == 5) | (slot == 6), from_lo, out)

    one = slot == 6
    strip[PR] = jnp.where(keep, join(PR, roll(a, 2, 1), roll(l, 5, 1)), zero)
    strip[PI] = jnp.where(keep, join(PI, roll(a, -1, 1), roll(l, 3, 1)), zero)
    strip[PX] = join(PX, roll(a, -4, 1), jnp.where(one, roll(l, 2, 1), zero))
    strip[PY] = join(PY, roll(b, 2, 1), jnp.where(one, roll(l, 1, 1), zero))
    strip[PZ] = join(PZ, b, jnp.where(one, l, zero))
    strip[EP] = join(EP, roll(b, -2, 1), jnp.where(one, roll(l, -1, 1), zero))

    def layer(k, z):
        q = (pr, pi, px, py, pz, ep)[k]
        return jnp.concatenate([q[z], halo[k, z]], axis=0)

    c, s = sincos(layer(PZ, 14))
    up[0], up[1] = turned_back(c, s, layer(PR, 14), layer(PI, 14))
    for k in range(6):
        up[2 + k] = layer(k, 15)
    down[0] = layer(PR, 1)
    down[1] = layer(PI, 1)
    for k in range(6):
        down[2 + k] = layer(k, 0)
    c, s = sincos(strip[PZ])
    wr, wi = turned_back(c, s, strip[PR], strip[PI])
    out = jnp.where(group == 0, roll(wr, -8 * 14, 1), roll(wi, -8 * 13, 1))
    for k in range(6):
        out = jnp.where(group == 2 + k, roll(strip[k], 8 * (2 + k - 15), 1), out)
    up[8] = out
    out = jnp.where(group == 0, roll(strip[PR], -8, 1), strip[PI])
    for k in range(6):
        out = jnp.where(group == 2 + k, roll(strip[k], 8 * (2 + k), 1), out)
    down[8] = out


def advance_layer(centre, above, below_turned, trig, edge, epsilon, lane):
    r, i = centre
    cz, sz, cx, sx, cy, sy = trig
    lap_r = -6.0 * r + below_turned[0]
    lap_i = -6.0 * i + below_turned[1]
    t = turned(cz, sz, *above)
    lap_r, lap_i = lap_r + t[0], lap_i + t[1]
    t = turned(cx, sx, ahead_x(r), ahead_x(i))
    lap_r, lap_i = lap_r + t[0], lap_i + t[1]
    t = turned_back(cx, sx, r, i)
    lap_r, lap_i = lap_r + behind_x(t[0]), lap_i + behind_x(t[1])
    w = turned_back(cy, sy, r, i)
    fr, fi = r, i
    wr, wi = w
    if edge is not None:
        fr, fi = jnp.where(lane == 0, edge[0], r), jnp.where(lane == 0, edge[1], i)
        wr, wi = jnp.where(lane == 127, edge[0], wr), jnp.where(lane == 127, edge[1], wi)
    t = turned(cy, sy, roll(fr, -1, 1), roll(fi, -1, 1))
    lap_r, lap_i = lap_r + t[0], lap_i + t[1]
    lap_r, lap_i = lap_r + roll(wr, 1, 1), lap_i + roll(wi, 1, 1)
    gain = epsilon - (r * r + i * i)
    return r + time_step * (gain * r + lap_r), i + time_step * (gain * i + lap_i)


def compute(pr, pi, px, py, pz, ep, halo, strip, zlo, zhi, final_r, final_i, out,
            ar, ai, br, bi, trig, eps, nr, ni, mr, mi, ntrig, neps, er, ei, jx_edge):
    lane = iota((RX, LANES), 1)
    row = iota((RX, LANES), 0)
    slot = lane % 8
    group = lane // 8
    gx, gy, gz = (lax.axis_index(a) for a in ("gx", "gy", "gz"))

    def on(test):
        return jnp.where(test, 1, 0)

    x_hi, x_lo = on(gx < lax.axis_size("gx") - 1), on(gx > 0)
    y_hi, y_lo = on(gy < lax.axis_size("gy") - 1), on(gy > 0)
    z_hi, z_lo = on(gz < lax.axis_size("gz") - 1), on(gz > 0)
    keep_x = jnp.where(row < NX, 1, jnp.where(row < NX + 4, x_hi, x_lo))
    keep_xy = keep_x * jnp.where((slot >= 2) & (slot < 5), y_hi, jnp.where((slot >= 5) & (slot < 7), y_lo, 1))
    keep_z = jnp.where(group < 8, z_hi, z_lo)
    zero = jnp.zeros((RX, LANES), F32)

    def fill(z, carry):
        def layer(q, k):
            return jnp.concatenate([q[z], halo[k, z]], axis=0)

        ar[z + 2] = layer(pr, PR)
        ai[z + 2] = layer(pi, PI)
        for n, (q, k) in enumerate(((pz, PZ), (px, PX), (py, PY))):
            trig[2 * n, z + 2], trig[2 * n + 1, z + 2] = sincos(layer(q, k))
        eps[z + 2] = layer(ep, EP)
        return carry

    lax.fori_loop(0, NZ, fill, 0)
    for src, keep, outer, inner in ((zlo, z_lo, 0, 1), (zhi, z_hi, 19, 18)):
        ok = jnp.broadcast_to(keep, (RX, LANES)) > 0
        ar[outer] = jnp.where(ok, src[0], zero)
        ai[outer] = jnp.where(ok, src[1], zero)
        ar[inner] = jnp.where(ok, src[2], zero)
        ai[inner] = jnp.where(ok, src[3], zero)
        for n, k in enumerate((PZ, PX, PY)):
            trig[2 * n, inner], trig[2 * n + 1, inner] = sincos(src[2 + k])
        eps[inner] = src[2 + EP]
    trig[0, 0] = zero + 1.0
    trig[1, 0] = zero
    lo8 = zlo[8]
    hi8 = zhi[8]

    def beyond(k, outer):
        v = jnp.where(group == 0, roll(hi8, -8 * (2 + k), 1), roll(lo8, 8 * (15 - 2 - k), 1))
        if outer is not None:
            v = jnp.where(group == 1, roll(hi8, 8 * (1 - outer), 1), v)
            v = jnp.where(group == 14, roll(lo8, 8 * (14 - outer), 1), v)
        return v

    nr[0] = strip[PR]
    ni[0] = strip[PI]
    nr[1] = jnp.where(keep_z > 0, beyond(PR, 0), zero)
    ni[1] = jnp.where(keep_z > 0, beyond(PI, 1), zero)
    for n, k in enumerate((PZ, PX, PY)):
        ntrig[2 * n, 0], ntrig[2 * n + 1, 0] = sincos(strip[k])
        v = beyond(k, None)
        if k == PZ:
            v = jnp.where(group == 14, zero, v)
        ntrig[2 * n, 1], ntrig[2 * n + 1, 1] = sincos(v)
    neps[0] = strip[EP]
    neps[1] = beyond(EP, None)

    def edges(sr, si):
        for h in range(2):
            w = turned_back(ntrig[4, h], ntrig[5, h], sr[h], si[h])
            er[h] = jnp.where(slot == 1, roll(w[0], -5, 1), sr[h])
            ei[h] = jnp.where(slot == 1, roll(w[1], -5, 1), si[h])

    def step_strips(sr, si, halves):
        w = [turned_back(ntrig[0, h], ntrig[1, h], sr[h], si[h]) for h in range(2)]
        wr = [roll(v[0], 8, 1) for v in w]
        wi = [roll(v[1], 8, 1) for v in w]
        fr = [roll(sr[h], -8, 1) for h in range(2)]
        fi = [roll(si[h], -8, 1) for h in range(2)]
        results = []
        for h in halves:
            g = 1 - h
            below = (jnp.where(group == 0, wr[g], wr[h]), jnp.where(group == 0, wi[g], wi[h]))
            above = (jnp.where(group == 15, fr[g], fr[h]), jnp.where(group == 15, fi[g], fi[h]))
            v = advance_layer((sr[h], si[h]), above, below, [ntrig[k, h] for k in range(6)], None, neps[h], lane)
            keep = keep_xy if h == 0 else keep_xy * keep_z
            results.append([jnp.where(keep > 0, u, zero) for u in v])
        return results

    def step_layer(sr, si, k):
        inside = (k >= 2) & (k < 18)
        half = jnp.where(inside, 0, 1)
        shift = (126 - 8 * ((k + 14) % 16)) % 128
        edge = (pltpu.roll(er[half], shift, 1), pltpu.roll(ei[half], shift, 1))
        below = turned_back(trig[0, k - 1], trig[1, k - 1], sr[k - 1], si[k - 1])
        v = advance_layer((sr[k], si[k]), (sr[k + 1], si[k + 1]), below, [trig[n, k] for n in range(6)],
                          edge, eps[k], lane)
        return v, inside

    edges(nr, ni)

    def first(k, carry):
        v, inside = step_layer(ar, ai, k)
        ok = keep_x * jnp.where(inside, 1, jnp.where(k < 2, z_lo, z_hi)) > 0
        br[k] = jnp.where(ok, v[0], zero)
        bi[k] = jnp.where(ok, v[1], zero)
        return carry

    lax.fori_loop(1, 19, first, 0)
    for h, v in enumerate(step_strips(nr, ni, (0, 1))):
        mr[h], mi[h] = v
    edges(mr, mi)

    def second(k, carry):
        v, _ = step_layer(br, bi, k)
        ok = keep_x > 0
        ar[k] = jnp.where(ok, v[0], zero)
        ai[k] = jnp.where(ok, v[1], zero)
        final_r[k - 2] = v[0][:NX]
        final_i[k - 2] = v[1][:NX]
        return carry

    lax.fori_loop(2, 18, second, 0)
    (sr, si), = step_strips(mr, mi, (0,))
    nr[0] = sr
    ni[0] = si
    t = turned(ntrig[2, 0], ntrig[3, 0], ahead_x(sr), ahead_x(si))
    jx_edge[...] = sr * t[1] - si * t[0]
    triangle = jnp.where(iota((LANES, LANES), 0) <= iota((LANES, LANES), 1), 1.0, 0.0).astype(F32)

    def analyse(z, carry):
        r, i = ar[z + 2], ai[z + 2]
        shift = (126 - 8 * z) % 128
        t = turned(trig[2, z + 2], trig[3, z + 2], ahead_x(r), ahead_x(i))
        jx = r * t[1] - i * t[0]
        fr = jnp.where(lane == 0, pltpu.roll(nr[0], shift, 1), r)
        fi = jnp.where(lane == 0, pltpu.roll(ni[0], shift, 1), i)
        t = turned(trig[4, z + 2], trig[5, z + 2], roll(fr, -1, 1), roll(fi, -1, 1))
        jy = r * t[1] - i * t[0]
        jx_next = roll(jnp.where(lane == 0, pltpu.roll(jx_edge[...], shift, 1), jx), -1, 1)
        circulation = (jx + ahead_x(jy) - jx_next - jy)[:NX]
        sums = jnp.dot(jx[:NX], triangle, precision=lax.Precision.HIGHEST, preferred_element_type=F32)
        for j in range(NX // TILE):
            out[j, z] = circulation[j * TILE:(j + 1) * TILE]
            out[j, NZ + z] = sums[j * TILE:(j + 1) * TILE]
        return carry

    lax.fori_loop(0, NZ, analyse, 0)


def finish(got, circulation, flux):
    def body(z, carry):
        before = jnp.zeros((TILE, 1), F32)
        for j in range(got.shape[0]):
            circulation[z, :, j * LANES:(j + 1) * LANES] = got[j, z]
            v = got[j, NZ + z]
            flux[z, :, j * LANES:(j + 1) * LANES] = v + before
            before = before + v[:, LANES - 1:]
        return carry

    lax.fori_loop(0, NZ, body, 0)


def spec(*shape):
    return jax.ShapeDtypeStruct(shape, F32)


def call(body, outs, *args, scratch=(), smem=0):
    memory = [pl.BlockSpec(memory_space=pltpu.SMEM if k < smem else pltpu.VMEM) for k in range(len(args))]
    return pl.pallas_call(
        body, out_shape=outs, in_specs=memory, scratch_shapes=list(scratch),
        out_specs=jax.tree.map(lambda _: pl.BlockSpec(memory_space=pltpu.VMEM), outs), name=body.__name__,
        compiler_params=pltpu.CompilerParams(vmem_limit_bytes=48 * 2**20),
    )(*args)


def exchange(up, down, axis):
    size = lax.axis_size(axis)
    forward = [(k, (k + 1) % size) for k in range(size)]
    return lax.ppermute(up, axis, forward), lax.ppermute(down, axis, [(b, a) for a, b in forward])


def shards(pr, pi, pz, px, py, material, levels):
    layers = lambda n: pltpu.VMEM((n, RX, LANES), F32)
    ep, up, down = call(pack_x, (spec(NZ, NX, NY), spec(NZ, TILE, LANES), spec(NZ, 2 * TILE, LANES)),
                        levels, pr, pi, px, py, pz, material, smem=1)
    lo, hi = exchange(up, down, "gx")
    fields = (pr, pi, px, py, pz, ep)
    halo, own, up, down = call(
        pack_y, (spec(6, NZ, TILE, LANES), spec(6, RX, LANES), spec(RX, LANES), spec(2, RX, LANES)), *fields, lo, hi)
    lo, hi = exchange(up, down, "gy")
    strip, up, down = call(pack_z, (spec(6, RX, LANES), spec(9, RX, LANES), spec(9, RX, LANES)),
                           *fields, halo, own, lo, hi)
    lo, hi = exchange(up, down, "gz")
    parts = lax.axis_size("gy")
    final_r, final_i, out = call(
        compute, (spec(NZ, NX, NY), spec(NZ, NX, NY), spec(parts, 2 * NZ, TILE, LANES)),
        *fields, halo, strip, lo, hi,
        scratch=[layers(20)] * 4 + [pltpu.VMEM((6, 20, RX, LANES), F32), layers(20)] + [layers(2)] * 4
        + [pltpu.VMEM((6, 2, RX, LANES), F32), layers(2), layers(2), layers(2), pltpu.VMEM((RX, LANES), F32)])
    got = lax.all_to_all(out, "gy", 0, 0, tiled=True)
    circulation, flux = call(finish, (spec(NZ, TILE, parts * LANES), spec(NZ, TILE, parts * LANES)), got)
    return final_r, final_i, circulation, flux


def solution(mesh):
    block = P("gz", "gx", "gy")
    slab = P("gz", ("gx", "gy"), None)
    return jax.shard_map(shards, mesh=mesh, in_specs=(block,) * 6 + (P(),),
                         out_specs=(block, block, slab, slab), check_vma=False)
```

```python
import jax
import jax.numpy as jnp
from jax import lax
from jax.experimental import pallas as pl
from jax.experimental.pallas import tpu as pltpu
from jax.sharding import PartitionSpec as P


LEVELS = 8
time_step = 0.15

F32 = jnp.float32
LANES = 128
TILE = 8
NZ, NX, NY = 16, 64, 128
RX = NX + TILE
PR, PI, PX, PY, PZ, EP = range(6)

SIN = (1.0, -0.16666658222675323, 0.008333050645887852, -0.00019809069635812193, 2.6052216526295524e-06)
COS = (-0.5, 0.0416666604578495, -0.0013888651737943292, 2.4774621124379337e-05, -2.6298400257473986e-07)


def sincos(phase):
    half = phase * 0.5
    u = half * half
    s = SIN[4]
    for k in (3, 2, 1, 0):
        s = s * u + SIN[k]
    s = s * half
    c = COS[4]
    for k in (3, 2, 1, 0):
        c = c * u + COS[k]
    c = c * u + 1.0
    return (c - s) * (c + s), (s + s) * c


def iota(shape, dim):
    return lax.broadcasted_iota(jnp.int32, shape, dim)


def roll(v, shift, axis):
    return pltpu.roll(v, shift % v.shape[axis], axis)


def ahead_x(v):
    return pltpu.roll(v, RX - 1, 0)


def behind_x(v):
    return pltpu.roll(v, 1, 0)


def turned(c, s, r, i):
    return c * r - s * i, c * i + s * r


def turned_back(c, s, r, i):
    return c * r + s * i, c * i - s * r


def row_up(a, row):
    pr, pi, px, py, pz, ep = a
    c, s = sincos(px)
    wr, wi = turned_back(c, s, pr, pi)
    last = row == 6
    pr = jnp.where(last, wr, pr)
    pi = jnp.where(last, wi, pi)
    out = roll(pr, 2, 0)
    out = jnp.where(row >= 2, roll(pi, 4, 0), out)
    out = jnp.where(row == 4, roll(px, 5, 0), out)
    out = jnp.where(row == 5, roll(py, 6, 0), out)
    out = jnp.where(row == 6, roll(pz, 7, 0), out)
    return jnp.where(row == 7, ep, out)


def row_down(a, row):
    pr, pi, px, py, pz, ep = a
    first = jnp.where(row < 3, pr, jnp.where(row < 6, roll(pi, 3, 0), roll(px, 6, 0)))
    second = jnp.where(row < 2, py, jnp.where(row < 4, roll(pz, 2, 0), roll(ep, 4, 0)))
    return first, second


def scaled_levels(levels):
    return [1.0 + time_step * (levels[k] - 6.0) for k in range(LEVELS)]


def material_gain(m, values):
    e = jnp.full(m.shape, values[LEVELS - 1], F32)
    for k in range(LEVELS - 1):
        e = jnp.where(m == k, values[k], e)
    return e


def start_copies(pairs, sems):
    copies = [pltpu.make_async_copy(a, b, sems.at[n]) for n, (a, b) in enumerate(pairs)]
    for copy in copies:
        copy.start()
    return copies


def pack_x(levels_in, pr, pi, px, py, pz, mat, up, down, levels, top, low, top_mat, low_mat, sems):
    fields = (pr, pi, px, py, pz)
    pairs = [(levels_in, levels)]
    pairs += [(q.at[:, pl.ds(NX - TILE, TILE), :], top.at[k]) for k, q in enumerate(fields)]
    pairs += [(q.at[:, pl.ds(0, TILE), :], low.at[k]) for k, q in enumerate(fields)]
    pairs += [(mat.at[:, pl.ds(NX - TILE, TILE), :], top_mat), (mat.at[:, pl.ds(0, TILE), :], low_mat)]
    for copy in start_copies(pairs, sems):
        copy.wait()
    row = iota((TILE, LANES), 0)
    values = scaled_levels(levels)

    def body(z, carry):
        up[z] = row_up([top[k, z] for k in range(5)] + [material_gain(top_mat[z], values)], row)
        first, second = row_down([low[k, z] for k in range(5)] + [material_gain(low_mat[z], values)], row)
        down[z, :TILE, :] = first
        down[z, TILE:, :] = second
        return carry

    lax.fori_loop(0, NZ, body, 0, unroll=2)


def prepare(levels_in, pr_in, pi_in, px_in, py_in, pz_in, mat_in, pr, pi, ep, trig, own, up, down,
            levels, px, py, pz, mat, sems):
    pairs = [(levels_in, levels), (mat_in, mat), (pz_in, pz), (px_in, px), (py_in, py), (pr_in, pr), (pi_in, pi)]
    copies = start_copies(pairs, sems)
    copies[0].wait()
    copies[1].wait()
    values = scaled_levels(levels)

    def gains(z, carry):
        ep[z] = material_gain(mat[z], values)
        return carry

    lax.fori_loop(0, NZ, gains, 0)
    for n, q in enumerate((pz, px, py)):
        copies[2 + n].wait()

        def angles(z, carry):
            trig[2 * n, z], trig[2 * n + 1, z] = sincos(q[z])
            return carry

        lax.fori_loop(0, NZ, angles, 0)
    copies[5].wait()
    copies[6].wait()
    group = iota((NX, LANES), 1) // 8
    for k, q in enumerate((pr, pi, px, py, pz, ep)):
        acc = jnp.zeros((NX, LANES), F32)
        for z in range(NZ):
            acc = jnp.where(group == z, roll(q[z], 8 * z - 126, 1), acc)
        own[k] = acc
    up[0], up[1] = turned_back(trig[0, 14], trig[1, 14], pr[14], pi[14])
    down[0] = pr[1]
    down[1] = pi[1]
    for k, q in enumerate((pr, pi, px, py, pz, ep)):
        up[2 + k] = q[15]
        down[2 + k] = q[0]


def pack_y(own_in, lo, hi, halo, own, up, down):
    row = iota((TILE, LANES), 0)
    gx = lax.axis_index("gx")
    keep = jnp.where(row < 4, jnp.where(gx < lax.axis_size("gx") - 1, 1, 0), jnp.where(gx > 0, 1, 0)) > 0
    low_rows = row >= 6
    last = row == 7
    group = iota((TILE, LANES), 1) // 8
    acc = [jnp.zeros((TILE, LANES), F32) for _ in range(6)]
    for z in range(NZ):
        l = lo[z]
        a = hi[z, :TILE, :]
        b = hi[z, TILE:, :]
        zero = jnp.zeros_like(l)
        tiles = (
            jnp.where(keep, jnp.where(low_rows, roll(l, 6, 0), a), zero),
            jnp.where(keep, jnp.where(low_rows, roll(l, 4, 0), roll(a, -3, 0)), zero),
            jnp.where(last, roll(l, 3, 0), jnp.where(row < 2, roll(a, -6, 0), zero)),
            jnp.where(last, roll(l, 2, 0), jnp.where(row < 2, b, zero)),
            jnp.where(last, roll(l, 1, 0), jnp.where(row < 2, roll(b, -2, 0), zero)),
            jnp.where(last, l, jnp.where(row < 2, roll(b, -4, 0), zero)),
        )
        for k, tile in enumerate(tiles):
            halo[k, z] = tile
            acc[k] = jnp.where(group == z, roll(tile, 8 * z - 126, 1), acc[k])
    columns = []
    for k in range(6):
        v = jnp.concatenate([own_in[k], acc[k]], axis=0)
        own[k] = v
        columns.append(v)
    slot = iota((RX, LANES), 1) % 8
    vr, vi, vx, vy, vz, ve = columns
    c, s = sincos(vy)
    wr, wi = turned_back(c, s, vr, vi)
    ur = jnp.where(slot == 0, wr, vr)
    ui = jnp.where(slot == 0, wi, vi)
    out = jnp.where(slot < 2, ur, roll(ui, 2, 1))
    out = jnp.where(slot == 4, roll(vx, 3, 1), out)
    out = jnp.where(slot == 5, roll(vy, 4, 1), out)
    out = jnp.where(slot == 6, roll(vz, 5, 1), out)
    out = jnp.where(slot == 7, roll(ve, 6, 1), out)
    up[...] = out
    down[0] = jnp.where(slot < 3, roll(vr, -2, 1), jnp.where(slot < 6, roll(vi, 1, 1), roll(vx, 4, 1)))
    down[1] = jnp.where(slot < 2, roll(vy, -2, 1), jnp.where(slot < 4, vz, roll(ve, 2, 1)))


def tall(q, h, z):
    return jnp.concatenate([q[z], h[z]], axis=0)


def angles_at(trig, trig_halo, n, z):
    return jnp.concatenate([trig[n, z], trig_halo[n, z]], axis=0)


def advance(centre, above, below_turned, trig, edge, gain, lane):
    r, i = centre
    cz, sz, cx, sx, cy, sy = trig
    t = turned(cx, sx, ahead_x(r), ahead_x(i))
    w = turned_back(cx, sx, r, i)
    sum_r, sum_i = t[0] + behind_x(w[0]), t[1] + behind_x(w[1])
    if below_turned is not None:
        sum_r, sum_i = sum_r + below_turned[0], sum_i + below_turned[1]
    if above is not None:
        t = turned(cz, sz, *above)
        sum_r, sum_i = sum_r + t[0], sum_i + t[1]
    fr, fi = r, i
    wr, wi = turned_back(cy, sy, r, i)
    if edge is not None:
        fr, fi = jnp.where(lane == 0, edge[0], r), jnp.where(lane == 0, edge[1], i)
        wr, wi = jnp.where(lane == 127, edge[0], wr), jnp.where(lane == 127, edge[1], wi)
    t = turned(cy, sy, roll(fr, -1, 1), roll(fi, -1, 1))
    sum_r, sum_i = sum_r + t[0] + roll(wr, 1, 1), sum_i + t[1] + roll(wi, 1, 1)
    gain = gain - time_step * (r * r + i * i)
    return gain * r + time_step * sum_r, gain * i + time_step * sum_i


def begin(pr, pi, ep, trig, halo, trig_halo, br, bi):
    lane = iota((RX, LANES), 1)
    zero = jnp.zeros((RX, LANES), F32)

    def angles(z, carry):
        for n, k in enumerate((PZ, PX, PY)):
            trig_halo[2 * n, z], trig_halo[2 * n + 1, z] = sincos(halo[k, z])
        return carry

    lax.fori_loop(0, NZ, angles, 0)
    none = (zero, zero)

    def layer(z):
        return tall(pr, halo.at[PR], z), tall(pi, halo.at[PI], z)

    def one(z, above, below):
        t = [angles_at(trig, trig_halo, n, z) for n in range(6)]
        if below is not None:
            below = turned_back(angles_at(trig, trig_halo, 0, below), angles_at(trig, trig_halo, 1, below),
                                *layer(below))
        if above is not None:
            above = layer(above)
        br[z], bi[z] = advance(layer(z), above, below, t, none, tall(ep, halo.at[EP], z), lane)

    one(0, 1, None)

    def body(z, carry):
        one(z, z + 1, z - 1)
        return carry

    lax.fori_loop(1, NZ - 1, body, 0)
    one(NZ - 1, None, NZ - 2)


def pack_edges(trig_halo, halo, own, lo, hi, strip, up, down):
    lane = iota((RX, LANES), 1)
    slot = lane % 8
    group = lane // 8
    gy = lax.axis_index("gy")
    keep = jnp.where((slot >= 2) & (slot < 5), jnp.where(gy < lax.axis_size("gy") - 1, 1, 0),
                     jnp.where((slot >= 5) & (slot < 7), jnp.where(gy > 0, 1, 0), 1)) > 0
    l = lo[...]
    a = hi[0]
    b = hi[1]
    zero = jnp.zeros_like(l)

    def join(k, from_hi, from_lo):
        v = own[k]
        out = jnp.where(slot < 2, v, roll(v, 5, 1))
        out = jnp.where((slot >= 2) & (slot < 5), from_hi, out)
        return jnp.where((slot == 5) | (slot == 6), from_lo, out)

    one = slot == 6
    strip[PR] = jnp.where(keep, join(PR, roll(a, 2, 1), roll(l, 5, 1)), zero)
    strip[PI] = jnp.where(keep, join(PI, roll(a, -1, 1), roll(l, 3, 1)), zero)
    strip[PX] = join(PX, roll(a, -4, 1), jnp.where(one, roll(l, 2, 1), zero))
    strip[PY] = join(PY, roll(b, 2, 1), jnp.where(one, roll(l, 1, 1), zero))
    strip[PZ] = join(PZ, b, jnp.where(one, l, zero))
    strip[EP] = join(EP, roll(b, -2, 1), jnp.where(one, roll(l, -1, 1), zero))
    up[0], up[1] = turned_back(trig_halo[0, 14], trig_halo[1, 14], halo[PR, 14], halo[PI, 14])
    down[0] = halo[PR, 1]
    down[1] = halo[PI, 1]
    for k in range(6):
        up[2 + k] = halo[k, 15]
        down[2 + k] = halo[k, 0]
    c, s = sincos(strip[PZ])
    wr, wi = turned_back(c, s, strip[PR], strip[PI])
    out = jnp.where(group == 0, roll(wr, -8 * 14, 1), roll(wi, -8 * 13, 1))
    for k in range(6):
        out = jnp.where(group == 2 + k, roll(strip[k], 8 * (2 + k - 15), 1), out)
    for t in range(RX // TILE):
        up[8 + t] = out[t * TILE:(t + 1) * TILE]
    out = jnp.where(group == 0, roll(strip[PR], -8, 1), strip[PI])
    for k in range(6):
        out = jnp.where(group == 2 + k, roll(strip[k], 8 * (2 + k), 1), out)
    for t in range(RX // TILE):
        down[8 + t] = out[t * TILE:(t + 1) * TILE]


def shift_of(group):
    return (126 - 8 * group) % 128


def on(test):
    return jnp.where(test, 1, 0)


def inside_masks():
    row = iota((RX, LANES), 0)
    slot = iota((RX, LANES), 1) % 8
    gx, gy = lax.axis_index("gx"), lax.axis_index("gy")
    keep_x = jnp.where(row < NX, 1, jnp.where(row < NX + 4, on(gx < lax.axis_size("gx") - 1), on(gx > 0)))
    keep_y = jnp.where((slot >= 2) & (slot < 5), on(gy < lax.axis_size("gy") - 1),
                       jnp.where((slot >= 5) & (slot < 7), on(gy > 0), 1))
    return keep_x, keep_x * keep_y


def edge_columns(slot, ntrig, r, i):
    wr, wi = turned_back(ntrig[4], ntrig[5], r, i)
    return jnp.where(slot == 1, roll(wr, -5, 1), r), jnp.where(slot == 1, roll(wi, -5, 1), i)


def analyse(z, r, i, trig_x, trig_y, columns, jx_column, lane, triangle, out):
    shift = shift_of(z)
    t = turned(*trig_x, ahead_x(r), ahead_x(i))
    jx = r * t[1] - i * t[0]
    fr = jnp.where(lane == 0, roll_by(columns[0], shift), r)
    fi = jnp.where(lane == 0, roll_by(columns[1], shift), i)
    t = turned(*trig_y, roll(fr, -1, 1), roll(fi, -1, 1))
    jy = r * t[1] - i * t[0]
    jx_next = roll(jnp.where(lane == 0, roll_by(jx_column, shift), jx), -1, 1)
    circulation = (jx + ahead_x(jy) - jx_next - jy)[:NX]
    sums = jnp.dot(jx[:NX], triangle, precision=lax.Precision.HIGHEST, preferred_element_type=F32)
    for j in range(NX // TILE):
        out[j, z] = circulation[j * TILE:(j + 1) * TILE]
        out[j, NZ + z] = sums[j * TILE:(j + 1) * TILE]


def roll_by(v, shift):
    return pltpu.roll(v, shift, 1)


def triangle_of():
    return jnp.where(iota((LANES, LANES), 0) <= iota((LANES, LANES), 1), 1.0, 0.0).astype(F32)


def interior(pr_in, pi_in, ep, trig, halo, trig_halo, strip, ntrig, cr, ci, final_r, final_i, out,
             er, ei, nr, ni, jx_edge):
    lane = iota((RX, LANES), 1)
    slot = lane % 8
    keep_x, keep_xy = inside_masks()
    zero = jnp.zeros((RX, LANES), F32)
    for n, k in enumerate((PZ, PX, PY)):
        ntrig[2 * n], ntrig[2 * n + 1] = sincos(strip[k])
    nt = lambda: [ntrig[n] for n in range(6)]
    er[...], ei[...] = edge_columns(slot, ntrig, strip[PR], strip[PI])

    def fix(z, carry):
        shift = shift_of(z)
        xr, xi = roll_by(er[...], shift), roll_by(ei[...], shift)
        cy, sy = angles_at(trig, trig_halo, 4, z), angles_at(trig, trig_halo, 5, z)
        hr, hi = turned(cy, sy, roll(xr, -1, 1), roll(xi, -1, 1))
        lr, li = roll(xr, 1, 1), roll(xi, 1, 1)
        r = pr_in[z] + time_step * jnp.where(lane == 127, hr, jnp.where(lane == 0, lr, zero))
        i = pi_in[z] + time_step * jnp.where(lane == 127, hi, jnp.where(lane == 0, li, zero))
        cr[z] = jnp.where(keep_x > 0, r, zero)
        ci[z] = jnp.where(keep_x > 0, i, zero)
        return carry

    lax.fori_loop(0, NZ, fix, 0)

    def strips(r, i):
        w = turned_back(ntrig[0], ntrig[1], r, i)
        v = advance((r, i), (roll(r, -8, 1), roll(i, -8, 1)), (roll(w[0], 8, 1), roll(w[1], 8, 1)), nt(), None,
                    strip[EP], lane)
        return jnp.where(keep_xy > 0, v[0], zero), jnp.where(keep_xy > 0, v[1], zero)

    mr, mi = strips(strip[PR], strip[PI])
    er[...], ei[...] = edge_columns(slot, ntrig, mr, mi)
    r, i = strips(mr, mi)
    nr[...] = r
    ni[...] = i
    t = turned(ntrig[2], ntrig[3], ahead_x(r), ahead_x(i))
    jx_edge[...] = r * t[1] - i * t[0]
    triangle = triangle_of()

    def second(z, carry):
        last_layer(z, (cr[z], ci[z]), (cr[z + 1], ci[z + 1]), (cr[z - 1], ci[z - 1]), ep, trig, halo, trig_halo,
                   (er[...], ei[...]), (nr[...], ni[...]), jx_edge[...], keep_x, lane, triangle,
                   final_r, final_i, out, None)
        return carry

    lax.fori_loop(2, NZ - 2, second, 0)


def last_layer(z, centre, above, below, ep, trig, halo, trig_halo, edges, columns, jx_column, keep_x, lane,
               triangle, final_r, final_i, out, below_turned):
    t = [angles_at(trig, trig_halo, n, z) for n in range(6)]
    if below_turned is None:
        below_turned = turned_back(angles_at(trig, trig_halo, 0, z - 1), angles_at(trig, trig_halo, 1, z - 1), *below)
    shift = shift_of(z)
    edge = roll_by(edges[0], shift), roll_by(edges[1], shift)
    r, i = advance(centre, above, below_turned, t, edge, tall(ep, halo.at[EP], z), lane)
    zero = jnp.zeros((RX, LANES), F32)
    r = jnp.where(keep_x > 0, r, zero)
    i = jnp.where(keep_x > 0, i, zero)
    final_r[z] = r[:NX]
    final_i[z] = i[:NX]
    analyse(z, r, i, t[2:4], t[4:6], columns, jx_column, lane, triangle, out)


def boundary(pr, pi, ep, trig, halo, trig_halo, strip, ntrig0, cr, ci, some_r, some_i, some_out,
             zlo, zhi, elo, ehi, final_r, final_i, out, ntrig1):
    lane = iota((RX, LANES), 1)
    slot = lane % 8
    group = lane // 8
    keep_x, keep_xy = inside_masks()
    gz = lax.axis_index("gz")
    z_hi, z_lo = on(gz < lax.axis_size("gz") - 1), on(gz > 0)
    keep_z = jnp.where(group < 8, z_hi, z_lo)
    zero = jnp.zeros((RX, LANES), F32)
    final_r[2:NZ - 2] = some_r[2:NZ - 2]
    final_i[2:NZ - 2] = some_i[2:NZ - 2]
    for j in range(NX // TILE):
        out[j, 2:NZ - 2] = some_out[j, 2:NZ - 2]
        out[j, NZ + 2:2 * NZ - 2] = some_out[j, NZ + 2:2 * NZ - 2]
    lo8 = jnp.concatenate([elo[8 + t] for t in range(RX // TILE)], axis=0)
    hi8 = jnp.concatenate([ehi[8 + t] for t in range(RX // TILE)], axis=0)

    def beyond(k, outer):
        v = jnp.where(group == 0, roll(hi8, -8 * (2 + k), 1), roll(lo8, 8 * (15 - 2 - k), 1))
        if outer is not None:
            v = jnp.where(group == 1, roll(hi8, 8 * (1 - outer), 1), v)
            v = jnp.where(group == 14, roll(lo8, 8 * (14 - outer), 1), v)
        return v

    for n, k in enumerate((PZ, PX, PY)):
        v = beyond(k, None)
        if k == PZ:
            v = jnp.where(group == 14, zero, v)
        ntrig1[2 * n], ntrig1[2 * n + 1] = sincos(v)
    trigs = (ntrig0, ntrig1)
    gains = (strip[EP], beyond(EP, None))

    def step_strips(halves, wanted):
        w = [turned_back(trigs[h][0], trigs[h][1], *halves[h]) for h in range(2)]
        results = []
        for h in wanted:
            g = 1 - h
            below = [jnp.where(group == 0, roll(w[g][n], 8, 1), roll(w[h][n], 8, 1)) for n in range(2)]
            above = [jnp.where(group == 15, roll(halves[g][n], -8, 1), roll(halves[h][n], -8, 1)) for n in range(2)]
            v = advance(halves[h], above, below, [trigs[h][n] for n in range(6)], None, gains[h], lane)
            keep = keep_xy if h == 0 else keep_xy * keep_z
            results.append([jnp.where(keep > 0, u, zero) for u in v])
        return results

    halves = ((strip[PR], strip[PI]),
              (jnp.where(keep_z > 0, beyond(PR, 0), zero), jnp.where(keep_z > 0, beyond(PI, 1), zero)))
    beyond_edge = edge_columns(slot, ntrig1, *halves[1])
    middle = step_strips(halves, (0, 1))
    edges = edge_columns(slot, ntrig0, *middle[0])
    (columns,) = step_strips(middle, (0,))
    t = turned(ntrig0[2], ntrig0[3], ahead_x(columns[0]), ahead_x(columns[1]))
    jx_column = columns[0] * t[1] - columns[1] * t[0]

    ok_lo = jnp.broadcast_to(z_lo, (RX, LANES)) > 0
    ok_hi = jnp.broadcast_to(z_hi, (RX, LANES)) > 0

    def got(main, tiles, n):
        return jnp.concatenate([main[n], tiles[n]], axis=0)

    def angles(main, tiles):
        found = []
        for k in (PZ, PX, PY):
            found += list(sincos(got(main, tiles, 2 + k)))
        return found

    def own(z):
        return tall(pr, halo.at[PR], z), tall(pi, halo.at[PI], z)

    def masked(ok, v):
        return tuple(jnp.where(ok, u, zero) for u in v)

    def at(z, n):
        return angles_at(trig, trig_halo, n, z)

    t_lo = angles(zlo, elo)
    outer = masked(ok_lo, (got(zlo, elo, 0), got(zlo, elo, 1)))
    inner = masked(ok_lo, (got(zlo, elo, 2), got(zlo, elo, 3)))
    edge = roll_by(beyond_edge[0], shift_of(15)), roll_by(beyond_edge[1], shift_of(15))
    v = masked(ok_lo & (keep_x > 0), advance(inner, own(0), outer, t_lo, edge, got(zlo, elo, 2 + EP), lane))
    w = turned_back(t_lo[0], t_lo[1], *inner)
    first = masked(keep_x > 0, (cr[0] + time_step * w[0], ci[0] + time_step * w[1]))
    below = turned_back(t_lo[0], t_lo[1], *v)
    triangle = triangle_of()
    common = (ep, trig, halo, trig_halo, edges, columns, jx_column, keep_x, lane, triangle, final_r, final_i, out)
    last_layer(0, first, (cr[1], ci[1]), None, *common, below)
    last_layer(1, (cr[1], ci[1]), (cr[2], ci[2]), first, *common, None)
    t_hi = angles(zhi, ehi)
    outer = masked(ok_hi, (got(zhi, ehi, 0), got(zhi, ehi, 1)))
    inner = masked(ok_hi, (got(zhi, ehi, 2), got(zhi, ehi, 3)))
    edge = roll_by(beyond_edge[0], shift_of(0)), roll_by(beyond_edge[1], shift_of(0))
    below = turned_back(at(15, 0), at(15, 1), *own(15))
    v = masked(ok_hi & (keep_x > 0), advance(inner, outer, below, t_hi, edge, got(zhi, ehi, 2 + EP), lane))
    w = turned(at(15, 0), at(15, 1), *inner)
    final = masked(keep_x > 0, (cr[15] + time_step * w[0], ci[15] + time_step * w[1]))
    last_layer(14, (cr[14], ci[14]), final, (cr[13], ci[13]), *common, None)
    last_layer(15, final, v, (cr[14], ci[14]), *common, None)


def finish(got, circulation, flux):
    def body(z, carry):
        before = jnp.zeros((TILE, 1), F32)
        for j in range(got.shape[0]):
            circulation[z, :, j * LANES:(j + 1) * LANES] = got[j, z]
            v = got[j, NZ + z]
            flux[z, :, j * LANES:(j + 1) * LANES] = v + before
            before = before + v[:, LANES - 1:]
        return carry

    lax.fori_loop(0, NZ, body, 0)


def spec(*shape):
    return jax.ShapeDtypeStruct(shape, F32)


def call(body, outs, *args, scratch=(), hbm=0, room=32 * 2**20):
    memory = [pl.BlockSpec(memory_space=pltpu.HBM if k < hbm else pltpu.VMEM) for k in range(len(args))]
    return pl.pallas_call(
        body, out_shape=outs, in_specs=memory, scratch_shapes=list(scratch),
        out_specs=jax.tree.map(lambda _: pl.BlockSpec(memory_space=pltpu.VMEM), outs),
        compiler_params=pltpu.CompilerParams(vmem_limit_bytes=room),
    )(*args)


def exchange(up, down, axis):
    size = lax.axis_size(axis)
    forward = [(k, (k + 1) % size) for k in range(size)]
    lo = lax.ppermute(up, axis, forward)
    hi = lax.ppermute(down, axis, [(b, a) for a, b in forward])
    return lo, hi


def program(pr_in, pi_in, pz_in, px_in, py_in, material, levels):
    parts = lax.axis_size("gy")
    raw = (levels, pr_in, pi_in, px_in, py_in, pz_in, material)
    raw = tuple(pltpu.with_memory_space_constraint(a, pltpu.HBM) for a in raw)
    edge = spec(NZ, TILE, LANES)
    block, tall_block, strip_like = spec(NZ, NX, NY), spec(NZ, RX, LANES), spec(RX, LANES)
    scratch = lambda s, dtype=F32: pltpu.VMEM(s.shape, dtype)
    up, down = call(pack_x, (edge, spec(NZ, 2 * TILE, LANES)), *raw, hbm=7, scratch=[
        pltpu.SMEM((LEVELS,), F32), pltpu.VMEM((5, NZ, TILE, LANES), F32), pltpu.VMEM((5, NZ, TILE, LANES), F32),
        scratch(edge, jnp.int32), scratch(edge, jnp.int32), pltpu.SemaphoreType.DMA((13,))])
    lo, hi = exchange(up, down, "gx")
    pr, pi, ep, trig, own, zup, zdown = call(
        prepare, (block, block, block, spec(6, NZ, NX, NY), spec(6, NX, LANES), spec(8, NX, NY), spec(8, NX, NY)),
        *raw, hbm=7, scratch=[pltpu.SMEM((LEVELS,), F32), scratch(block), scratch(block), scratch(block),
                              scratch(block, jnp.int32), pltpu.SemaphoreType.DMA((7,))])
    zlo, zhi = exchange(zup, zdown, "gz")
    halo, own, up, down = call(
        pack_y, (spec(6, NZ, TILE, LANES), spec(6, RX, LANES), strip_like, spec(2, RX, LANES)), own, lo, hi)
    lo, hi = exchange(up, down, "gy")
    trig_halo, br, bi = call(begin, (spec(6, NZ, TILE, LANES), tall_block, tall_block), pr, pi, ep, trig, halo)
    strip, up, down = call(pack_edges, (spec(6, RX, LANES), spec(17, TILE, LANES), spec(17, TILE, LANES)),
                           trig_halo, halo, own, lo, hi)
    elo, ehi = exchange(up, down, "gz")
    out = spec(parts, 2 * NZ, TILE, LANES)
    ntrig, cr, ci, some_r, some_i, some_out = call(
        interior, (spec(6, RX, LANES), tall_block, tall_block, block, block, out),
        br, bi, ep, trig, halo, trig_halo, strip, scratch=[scratch(strip_like)] * 5)
    final_r, final_i, out = call(
        boundary, (block, block, out), pr, pi, ep, trig, halo, trig_halo, strip, ntrig, cr, ci,
        some_r, some_i, some_out, zlo, zhi, elo, ehi, scratch=[pltpu.VMEM((6, RX, LANES), F32)])
    got = lax.all_to_all(out, "gy", 0, 0, tiled=True)
    circulation, flux = call(finish, (spec(NZ, TILE, parts * LANES), spec(NZ, TILE, parts * LANES)), got)
    return final_r, final_i, circulation, flux


def solution(mesh):
    block = P("gz", "gx", "gy")
    slab = P("gz", ("gx", "gy"), None)
    return jax.shard_map(program, mesh=mesh, in_specs=(block,) * 6 + (P(),),
                         out_specs=(block, block, slab, slab), check_vma=False)
```

```python
import jax
import jax.numpy as jnp
from jax import lax
from jax.experimental import pallas as pl
from jax.experimental.pallas import tpu as pltpu
from jax.sharding import PartitionSpec as P


LEVELS = 8
time_step = 0.15

F32 = jnp.float32
LANES = 128
TILE = 8
NZ, NX, NY = 16, 64, 128
RX = NX + TILE
PR, PI, PX, PY, PZ, EP = range(6)
EARLY = ()
LATE = (4, 3, 5, 2, 6, 1, 7)

SIN = (1.0, -0.16666658222675323, 0.008333050645887852, -0.00019809069635812193, 2.6052216526295524e-06)
COS = (-0.5, 0.0416666604578495, -0.0013888651737943292, 2.4774621124379337e-05, -2.6298400257473986e-07)


def sincos(phase):
    half = phase * 0.5
    u = half * half
    s = SIN[4]
    for k in (3, 2, 1, 0):
        s = s * u + SIN[k]
    s = s * half
    c = COS[4]
    for k in (3, 2, 1, 0):
        c = c * u + COS[k]
    c = c * u + 1.0
    return (c - s) * (c + s), (s + s) * c


def iota(shape, dim):
    return lax.broadcasted_iota(jnp.int32, shape, dim)


def roll(v, shift, axis):
    return pltpu.roll(v, shift % v.shape[axis], axis)


def ahead_x(v):
    return pltpu.roll(v, RX - 1, 0)


def behind_x(v):
    return pltpu.roll(v, 1, 0)


def turned(c, s, r, i):
    return c * r - s * i, c * i + s * r


def turned_back(c, s, r, i):
    return c * r + s * i, c * i - s * r


def row_up(a, row):
    pr, pi, px, py, pz, ep = a
    c, s = sincos(px)
    wr, wi = turned_back(c, s, pr, pi)
    last = row == 6
    pr = jnp.where(last, wr, pr)
    pi = jnp.where(last, wi, pi)
    out = roll(pr, 2, 0)
    out = jnp.where(row >= 2, roll(pi, 4, 0), out)
    out = jnp.where(row == 4, roll(px, 5, 0), out)
    out = jnp.where(row == 5, roll(py, 6, 0), out)
    out = jnp.where(row == 6, roll(pz, 7, 0), out)
    return jnp.where(row == 7, ep, out)


def row_down(a, row):
    pr, pi, px, py, pz, ep = a
    first = jnp.where(row < 3, pr, jnp.where(row < 6, roll(pi, 3, 0), roll(px, 6, 0)))
    second = jnp.where(row < 2, py, jnp.where(row < 4, roll(pz, 2, 0), roll(ep, 4, 0)))
    return first, second


def scaled_levels(levels):
    return [1.0 + time_step * (levels[k] - 6.0) for k in range(LEVELS)]


def material_gain(m, values):
    e = jnp.full(m.shape, values[LEVELS - 1], F32)
    for k in range(LEVELS - 1):
        e = jnp.where(m == k, values[k], e)
    return e


def start_copies(pairs, sems):
    copies = [pltpu.make_async_copy(a, b, sems.at[n]) for n, (a, b) in enumerate(pairs)]
    for copy in copies:
        copy.start()
    return copies


def pack_x(levels_in, pr, pi, px, py, pz, mat, up, down, levels, top, low, top_mat, low_mat, sems):
    fields = (pr, pi, px, py, pz)
    pairs = [(levels_in, levels)]
    pairs += [(q.at[:, pl.ds(NX - TILE, TILE), :], top.at[k]) for k, q in enumerate(fields)]
    pairs += [(q.at[:, pl.ds(0, TILE), :], low.at[k]) for k, q in enumerate(fields)]
    pairs += [(mat.at[:, pl.ds(NX - TILE, TILE), :], top_mat), (mat.at[:, pl.ds(0, TILE), :], low_mat)]
    for copy in start_copies(pairs, sems):
        copy.wait()
    row = iota((TILE, LANES), 0)
    values = scaled_levels(levels)

    def body(z, carry):
        up[z] = row_up([top[k, z] for k in range(5)] + [material_gain(top_mat[z], values)], row)
        first, second = row_down([low[k, z] for k in range(5)] + [material_gain(low_mat[z], values)], row)
        down[z, :TILE, :] = first
        down[z, TILE:, :] = second
        return carry

    lax.fori_loop(0, NZ, body, 0, unroll=2)


def prepare(levels_in, pr_in, pi_in, px_in, py_in, pz_in, mat_in, pr, pi, ep, trig, own, up, down,
            levels, px, py, pz, mat, sems):
    pairs = [(levels_in, levels), (mat_in, mat), (pz_in, pz), (px_in, px), (py_in, py), (pr_in, pr), (pi_in, pi)]
    copies = start_copies(pairs, sems)
    copies[0].wait()
    copies[1].wait()
    values = scaled_levels(levels)

    def gains(z, carry):
        ep[z] = material_gain(mat[z], values)
        return carry

    lax.fori_loop(0, NZ, gains, 0)
    for n, q in enumerate((pz, px, py)):
        copies[2 + n].wait()

        def angles(z, carry):
            trig[2 * n, z], trig[2 * n + 1, z] = sincos(q[z])
            return carry

        lax.fori_loop(0, NZ, angles, 0)
    copies[5].wait()
    copies[6].wait()
    group = iota((NX, LANES), 1) // 8
    for k, q in enumerate((pr, pi, px, py, pz, ep)):
        acc = jnp.zeros((NX, LANES), F32)
        for z in range(NZ):
            acc = jnp.where(group == z, roll(q[z], 8 * z - 126, 1), acc)
        own[k] = acc
    up[0], up[1] = turned_back(trig[0, 14], trig[1, 14], pr[14], pi[14])
    down[0] = pr[1]
    down[1] = pi[1]
    for k, q in enumerate((pr, pi, px, py, pz, ep)):
        up[2 + k] = q[15]
        down[2 + k] = q[0]


def pack_y(own_in, lo, hi, halo, own, up, down):
    row = iota((TILE, LANES), 0)
    gx = lax.axis_index("gx")
    keep = jnp.where(row < 4, jnp.where(gx < lax.axis_size("gx") - 1, 1, 0), jnp.where(gx > 0, 1, 0)) > 0
    low_rows = row >= 6
    last = row == 7
    group = iota((TILE, LANES), 1) // 8
    acc = [jnp.zeros((TILE, LANES), F32) for _ in range(6)]
    for z in range(NZ):
        l = lo[z]
        a = hi[z, :TILE, :]
        b = hi[z, TILE:, :]
        zero = jnp.zeros_like(l)
        tiles = (
            jnp.where(keep, jnp.where(low_rows, roll(l, 6, 0), a), zero),
            jnp.where(keep, jnp.where(low_rows, roll(l, 4, 0), roll(a, -3, 0)), zero),
            jnp.where(last, roll(l, 3, 0), jnp.where(row < 2, roll(a, -6, 0), zero)),
            jnp.where(last, roll(l, 2, 0), jnp.where(row < 2, b, zero)),
            jnp.where(last, roll(l, 1, 0), jnp.where(row < 2, roll(b, -2, 0), zero)),
            jnp.where(last, l, jnp.where(row < 2, roll(b, -4, 0), zero)),
        )
        for k, tile in enumerate(tiles):
            halo[k, z] = tile
            acc[k] = jnp.where(group == z, roll(tile, 8 * z - 126, 1), acc[k])
    columns = []
    for k in range(6):
        v = jnp.concatenate([own_in[k], acc[k]], axis=0)
        own[k] = v
        columns.append(v)
    slot = iota((RX, LANES), 1) % 8
    vr, vi, vx, vy, vz, ve = columns
    c, s = sincos(vy)
    wr, wi = turned_back(c, s, vr, vi)
    ur = jnp.where(slot == 0, wr, vr)
    ui = jnp.where(slot == 0, wi, vi)
    out = jnp.where(slot < 2, ur, roll(ui, 2, 1))
    out = jnp.where(slot == 4, roll(vx, 3, 1), out)
    out = jnp.where(slot == 5, roll(vy, 4, 1), out)
    out = jnp.where(slot == 6, roll(vz, 5, 1), out)
    out = jnp.where(slot == 7, roll(ve, 6, 1), out)
    up[...] = out
    down[0] = jnp.where(slot < 3, roll(vr, -2, 1), jnp.where(slot < 6, roll(vi, 1, 1), roll(vx, 4, 1)))
    down[1] = jnp.where(slot < 2, roll(vy, -2, 1), jnp.where(slot < 4, vz, roll(ve, 2, 1)))


def tall(q, h, z):
    return jnp.concatenate([q[z], h[z]], axis=0)


def angles_at(trig, trig_halo, n, z):
    return jnp.concatenate([trig[n, z], trig_halo[n, z]], axis=0)


def advance(centre, above, below_turned, trig, edge, gain, lane):
    r, i = centre
    cz, sz, cx, sx, cy, sy = trig
    t = turned(cx, sx, ahead_x(r), ahead_x(i))
    w = turned_back(cx, sx, r, i)
    sum_r, sum_i = t[0] + behind_x(w[0]), t[1] + behind_x(w[1])
    if below_turned is not None:
        sum_r, sum_i = sum_r + below_turned[0], sum_i + below_turned[1]
    if above is not None:
        t = turned(cz, sz, *above)
        sum_r, sum_i = sum_r + t[0], sum_i + t[1]
    fr, fi = r, i
    wr, wi = turned_back(cy, sy, r, i)
    if edge is not None:
        fr, fi = jnp.where(lane == 0, edge[0], r), jnp.where(lane == 0, edge[1], i)
        wr, wi = jnp.where(lane == 127, edge[0], wr), jnp.where(lane == 127, edge[1], wi)
    t = turned(cy, sy, roll(fr, -1, 1), roll(fi, -1, 1))
    sum_r, sum_i = sum_r + t[0] + roll(wr, 1, 1), sum_i + t[1] + roll(wi, 1, 1)
    gain = gain - time_step * (r * r + i * i)
    return gain * r + time_step * sum_r, gain * i + time_step * sum_i


def begin(pr, pi, ep, trig, halo, trig_halo, br, bi):
    lane = iota((RX, LANES), 1)
    zero = jnp.zeros((RX, LANES), F32)

    def angles(z, carry):
        for n, k in enumerate((PZ, PX, PY)):
            trig_halo[2 * n, z], trig_halo[2 * n + 1, z] = sincos(halo[k, z])
        return carry

    lax.fori_loop(0, NZ, angles, 0)
    none = (zero, zero)

    def layer(z):
        return tall(pr, halo.at[PR], z), tall(pi, halo.at[PI], z)

    def one(z, above, below):
        t = [angles_at(trig, trig_halo, n, z) for n in range(6)]
        if below is not None:
            below = turned_back(angles_at(trig, trig_halo, 0, below), angles_at(trig, trig_halo, 1, below),
                                *layer(below))
        if above is not None:
            above = layer(above)
        br[z], bi[z] = advance(layer(z), above, below, t, none, tall(ep, halo.at[EP], z), lane)

    one(0, 1, None)

    def body(z, carry):
        one(z, z + 1, z - 1)
        return carry

    lax.fori_loop(1, NZ - 1, body, 0)
    one(NZ - 1, None, NZ - 2)


def pack_edges(trig_halo, halo, own, lo, hi, strip, up, down):
    lane = iota((RX, LANES), 1)
    slot = lane % 8
    group = lane // 8
    gy = lax.axis_index("gy")
    keep = jnp.where((slot >= 2) & (slot < 5), jnp.where(gy < lax.axis_size("gy") - 1, 1, 0),
                     jnp.where((slot >= 5) & (slot < 7), jnp.where(gy > 0, 1, 0), 1)) > 0
    l = lo[...]
    a = hi[0]
    b = hi[1]
    zero = jnp.zeros_like(l)

    def join(k, from_hi, from_lo):
        v = own[k]
        out = jnp.where(slot < 2, v, roll(v, 5, 1))
        out = jnp.where((slot >= 2) & (slot < 5), from_hi, out)
        return jnp.where((slot == 5) | (slot == 6), from_lo, out)

    one = slot == 6
    strip[PR] = jnp.where(keep, join(PR, roll(a, 2, 1), roll(l, 5, 1)), zero)
    strip[PI] = jnp.where(keep, join(PI, roll(a, -1, 1), roll(l, 3, 1)), zero)
    strip[PX] = join(PX, roll(a, -4, 1), jnp.where(one, roll(l, 2, 1), zero))
    strip[PY] = join(PY, roll(b, 2, 1), jnp.where(one, roll(l, 1, 1), zero))
    strip[PZ] = join(PZ, b, jnp.where(one, l, zero))
    strip[EP] = join(EP, roll(b, -2, 1), jnp.where(one, roll(l, -1, 1), zero))
    up[0], up[1] = turned_back(trig_halo[0, 14], trig_halo[1, 14], halo[PR, 14], halo[PI, 14])
    down[0] = halo[PR, 1]
    down[1] = halo[PI, 1]
    for k in range(6):
        up[2 + k] = halo[k, 15]
        down[2 + k] = halo[k, 0]
    c, s = sincos(strip[PZ])
    wr, wi = turned_back(c, s, strip[PR], strip[PI])
    out = jnp.where(group == 0, roll(wr, -8 * 14, 1), roll(wi, -8 * 13, 1))
    for k in range(6):
        out = jnp.where(group == 2 + k, roll(strip[k], 8 * (2 + k - 15), 1), out)
    for t in range(RX // TILE):
        up[8 + t] = out[t * TILE:(t + 1) * TILE]
    out = jnp.where(group == 0, roll(strip[PR], -8, 1), strip[PI])
    for k in range(6):
        out = jnp.where(group == 2 + k, roll(strip[k], 8 * (2 + k), 1), out)
    for t in range(RX // TILE):
        down[8 + t] = out[t * TILE:(t + 1) * TILE]


def shift_of(group):
    return (126 - 8 * group) % 128


def on(test):
    return jnp.where(test, 1, 0)


def inside_masks():
    row = iota((RX, LANES), 0)
    slot = iota((RX, LANES), 1) % 8
    gx, gy = lax.axis_index("gx"), lax.axis_index("gy")
    keep_x = jnp.where(row < NX, 1, jnp.where(row < NX + 4, on(gx < lax.axis_size("gx") - 1), on(gx > 0)))
    keep_y = jnp.where((slot >= 2) & (slot < 5), on(gy < lax.axis_size("gy") - 1),
                       jnp.where((slot >= 5) & (slot < 7), on(gy > 0), 1))
    return keep_x, keep_x * keep_y


def edge_columns(slot, ntrig, r, i):
    wr, wi = turned_back(ntrig[4], ntrig[5], r, i)
    return jnp.where(slot == 1, roll(wr, -5, 1), r), jnp.where(slot == 1, roll(wi, -5, 1), i)


def analyse(z, r, i, trig_x, trig_y, columns, jx_column, lane, triangle, out, spot, gap):
    shift = shift_of(z)
    t = turned(*trig_x, ahead_x(r), ahead_x(i))
    jx = r * t[1] - i * t[0]
    fr = jnp.where(lane == 0, roll_by(columns[0], shift), r)
    fi = jnp.where(lane == 0, roll_by(columns[1], shift), i)
    t = turned(*trig_y, roll(fr, -1, 1), roll(fi, -1, 1))
    jy = r * t[1] - i * t[0]
    jx_next = roll(jnp.where(lane == 0, roll_by(jx_column, shift), jx), -1, 1)
    circulation = (jx + ahead_x(jy) - jx_next - jy)[:NX]
    sums = jnp.dot(jx[:NX], triangle, precision=lax.Precision.HIGHEST, preferred_element_type=F32)
    for j in range(NX // TILE):
        away = (j + out.shape[0] - lax.axis_index("gy")) % out.shape[0]
        out[away, spot] = circulation[j * TILE:(j + 1) * TILE]
        out[away, spot + gap] = sums[j * TILE:(j + 1) * TILE]


def roll_by(v, shift):
    return pltpu.roll(v, shift, 1)


def triangle_of():
    return jnp.where(iota((LANES, LANES), 0) <= iota((LANES, LANES), 1), 1.0, 0.0).astype(F32)


def interior(pr_in, pi_in, ep, trig, halo, trig_halo, strip, ntrig, cr, ci, final_r, final_i, out,
             er, ei, nr, ni, jx_edge):
    lane = iota((RX, LANES), 1)
    slot = lane % 8
    keep_x, keep_xy = inside_masks()
    zero = jnp.zeros((RX, LANES), F32)
    for n, k in enumerate((PZ, PX, PY)):
        ntrig[2 * n], ntrig[2 * n + 1] = sincos(strip[k])
    nt = lambda: [ntrig[n] for n in range(6)]
    er[...], ei[...] = edge_columns(slot, ntrig, strip[PR], strip[PI])

    def fix(z, carry):
        shift = shift_of(z)
        xr, xi = roll_by(er[...], shift), roll_by(ei[...], shift)
        cy, sy = angles_at(trig, trig_halo, 4, z), angles_at(trig, trig_halo, 5, z)
        hr, hi = turned(cy, sy, roll(xr, -1, 1), roll(xi, -1, 1))
        lr, li = roll(xr, 1, 1), roll(xi, 1, 1)
        r = pr_in[z] + time_step * jnp.where(lane == 127, hr, jnp.where(lane == 0, lr, zero))
        i = pi_in[z] + time_step * jnp.where(lane == 127, hi, jnp.where(lane == 0, li, zero))
        cr[z] = jnp.where(keep_x > 0, r, zero)
        ci[z] = jnp.where(keep_x > 0, i, zero)
        return carry

    for z in range(NZ):
        fix(z, 0)

    def strips(r, i):
        w = turned_back(ntrig[0], ntrig[1], r, i)
        v = advance((r, i), (roll(r, -8, 1), roll(i, -8, 1)), (roll(w[0], 8, 1), roll(w[1], 8, 1)), nt(), None,
                    strip[EP], lane)
        return jnp.where(keep_xy > 0, v[0], zero), jnp.where(keep_xy > 0, v[1], zero)

    mr, mi = strips(strip[PR], strip[PI])
    er[...], ei[...] = edge_columns(slot, ntrig, mr, mi)
    r, i = strips(mr, mi)
    nr[...] = r
    ni[...] = i
    t = turned(ntrig[2], ntrig[3], ahead_x(r), ahead_x(i))
    jx_edge[...] = r * t[1] - i * t[0]
    triangle = triangle_of()

    def second(z, carry):
        last_layer(z, (cr[z], ci[z]), (cr[z + 1], ci[z + 1]), (cr[z - 1], ci[z - 1]), ep, trig, halo, trig_halo,
                   (er[...], ei[...]), (nr[...], ni[...]), jx_edge[...], keep_x, lane, triangle,
                   final_r, final_i, out, None, z - 2, NZ - 4)
        return carry

    for z in range(2, NZ - 2):
        second(z, 0)


def last_layer(z, centre, above, below, ep, trig, halo, trig_halo, edges, columns, jx_column, keep_x, lane,
               triangle, final_r, final_i, out, below_turned, spot, gap):
    t = [angles_at(trig, trig_halo, n, z) for n in range(6)]
    if below_turned is None:
        below_turned = turned_back(angles_at(trig, trig_halo, 0, z - 1), angles_at(trig, trig_halo, 1, z - 1), *below)
    shift = shift_of(z)
    edge = roll_by(edges[0], shift), roll_by(edges[1], shift)
    r, i = advance(centre, above, below_turned, t, edge, tall(ep, halo.at[EP], z), lane)
    zero = jnp.zeros((RX, LANES), F32)
    r = jnp.where(keep_x > 0, r, zero)
    i = jnp.where(keep_x > 0, i, zero)
    final_r[z] = r[:NX]
    final_i[z] = i[:NX]
    analyse(z, r, i, t[2:4], t[4:6], columns, jx_column, lane, triangle, out, spot, gap)


def boundary(pr, pi, ep, trig, halo, trig_halo, strip, ntrig0, cr, ci, some_r, some_i, middle_out,
             zlo, zhi, elo, ehi, final_r, final_i, out, ntrig1):
    lane = iota((RX, LANES), 1)
    slot = lane % 8
    group = lane // 8
    keep_x, keep_xy = inside_masks()
    gz = lax.axis_index("gz")
    z_hi, z_lo = on(gz < lax.axis_size("gz") - 1), on(gz > 0)
    keep_z = jnp.where(group < 8, z_hi, z_lo)
    zero = jnp.zeros((RX, LANES), F32)
    for away in range(out.shape[0]):
        out[away, 8:] = middle_out[away]
    final_r[2:NZ - 2] = some_r[2:NZ - 2]
    final_i[2:NZ - 2] = some_i[2:NZ - 2]
    lo8 = jnp.concatenate([elo[8 + t] for t in range(RX // TILE)], axis=0)
    hi8 = jnp.concatenate([ehi[8 + t] for t in range(RX // TILE)], axis=0)

    def beyond(k, outer):
        v = jnp.where(group == 0, roll(hi8, -8 * (2 + k), 1), roll(lo8, 8 * (15 - 2 - k), 1))
        if outer is not None:
            v = jnp.where(group == 1, roll(hi8, 8 * (1 - outer), 1), v)
            v = jnp.where(group == 14, roll(lo8, 8 * (14 - outer), 1), v)
        return v

    for n, k in enumerate((PZ, PX, PY)):
        v = beyond(k, None)
        if k == PZ:
            v = jnp.where(group == 14, zero, v)
        ntrig1[2 * n], ntrig1[2 * n + 1] = sincos(v)
    trigs = (ntrig0, ntrig1)
    gains = (strip[EP], beyond(EP, None))

    def step_strips(halves, wanted):
        w = [turned_back(trigs[h][0], trigs[h][1], *halves[h]) for h in range(2)]
        results = []
        for h in wanted:
            g = 1 - h
            below = [jnp.where(group == 0, roll(w[g][n], 8, 1), roll(w[h][n], 8, 1)) for n in range(2)]
            above = [jnp.where(group == 15, roll(halves[g][n], -8, 1), roll(halves[h][n], -8, 1)) for n in range(2)]
            v = advance(halves[h], above, below, [trigs[h][n] for n in range(6)], None, gains[h], lane)
            keep = keep_xy if h == 0 else keep_xy * keep_z
            results.append([jnp.where(keep > 0, u, zero) for u in v])
        return results

    halves = ((strip[PR], strip[PI]),
              (jnp.where(keep_z > 0, beyond(PR, 0), zero), jnp.where(keep_z > 0, beyond(PI, 1), zero)))
    beyond_edge = edge_columns(slot, ntrig1, *halves[1])
    middle = step_strips(halves, (0, 1))
    edges = edge_columns(slot, ntrig0, *middle[0])
    (columns,) = step_strips(middle, (0,))
    t = turned(ntrig0[2], ntrig0[3], ahead_x(columns[0]), ahead_x(columns[1]))
    jx_column = columns[0] * t[1] - columns[1] * t[0]

    ok_lo = jnp.broadcast_to(z_lo, (RX, LANES)) > 0
    ok_hi = jnp.broadcast_to(z_hi, (RX, LANES)) > 0

    def got(main, tiles, n):
        return jnp.concatenate([main[n], tiles[n]], axis=0)

    def angles(main, tiles):
        found = []
        for k in (PZ, PX, PY):
            found += list(sincos(got(main, tiles, 2 + k)))
        return found

    def own(z):
        return tall(pr, halo.at[PR], z), tall(pi, halo.at[PI], z)

    def masked(ok, v):
        return tuple(jnp.where(ok, u, zero) for u in v)

    def at(z, n):
        return angles_at(trig, trig_halo, n, z)

    t_lo = angles(zlo, elo)
    outer = masked(ok_lo, (got(zlo, elo, 0), got(zlo, elo, 1)))
    inner = masked(ok_lo, (got(zlo, elo, 2), got(zlo, elo, 3)))
    edge = roll_by(beyond_edge[0], shift_of(15)), roll_by(beyond_edge[1], shift_of(15))
    v = masked(ok_lo & (keep_x > 0), advance(inner, own(0), outer, t_lo, edge, got(zlo, elo, 2 + EP), lane))
    w = turned_back(t_lo[0], t_lo[1], *inner)
    first = masked(keep_x > 0, (cr[0] + time_step * w[0], ci[0] + time_step * w[1]))
    below = turned_back(t_lo[0], t_lo[1], *v)
    triangle = triangle_of()
    common = (ep, trig, halo, trig_halo, edges, columns, jx_column, keep_x, lane, triangle, final_r, final_i, out)
    last_layer(0, first, (cr[1], ci[1]), None, *common, below, 0, 4)
    last_layer(1, (cr[1], ci[1]), (cr[2], ci[2]), first, *common, None, 1, 4)
    t_hi = angles(zhi, ehi)
    outer = masked(ok_hi, (got(zhi, ehi, 0), got(zhi, ehi, 1)))
    inner = masked(ok_hi, (got(zhi, ehi, 2), got(zhi, ehi, 3)))
    edge = roll_by(beyond_edge[0], shift_of(0)), roll_by(beyond_edge[1], shift_of(0))
    below = turned_back(at(15, 0), at(15, 1), *own(15))
    v = masked(ok_hi & (keep_x > 0), advance(inner, outer, below, t_hi, edge, got(zhi, ehi, 2 + EP), lane))
    w = turned(at(15, 0), at(15, 1), *inner)
    final = masked(keep_x > 0, (cr[15] + time_step * w[0], ci[15] + time_step * w[1]))
    last_layer(14, (cr[14], ci[14]), final, (cr[13], ci[13]), *common, None, 2, 4)
    last_layer(15, final, v, (cr[14], ci[14]), *common, None, 3, 4)


ENDS = (0, 1, NZ - 2, NZ - 1)


def finish(*refs):
    parts = lax.axis_size("gy")
    got, (circulation, flux, ends, middle, full_c, full_f, sems) = refs[:-7], refs[-7:]
    me = lax.axis_index("gy")
    for k in range(parts):
        source = (me + parts - k) % parts
        if k in EARLY:
            ends[source] = got[len(EARLY) + k][...]
            middle[source] = got[EARLY.index(k)][...]
        else:
            ends[source] = got[len(EARLY) + k][:8]
            middle[source] = got[len(EARLY) + k][8:]

    def layer(pieces, spot, gap, z):
        before = jnp.zeros((TILE, 1), F32)
        for j in range(parts):
            full_c[z, :, j * LANES:(j + 1) * LANES] = pieces[j, spot]
            v = pieces[j, spot + gap]
            full_f[z, :, j * LANES:(j + 1) * LANES] = v + before
            before = before + v[:, LANES - 1:]

    copies = []

    def send(first):
        for a, b in ((full_c, circulation), (full_f, flux)):
            copies.append(pltpu.make_async_copy(a.at[pl.ds(first, 4)], b.at[pl.ds(first, 4)], sems.at[len(copies)]))
            copies[-1].start()

    for first in (4, 8, 0, 12):
        for z in range(first, first + 4):
            if z in ENDS:
                layer(ends, ENDS.index(z), 4, z)
            else:
                layer(middle, z - 2, NZ - 4, z)
        send(first)
    for copy in copies:
        copy.wait()


def spec(*shape):
    return jax.ShapeDtypeStruct(shape, F32)


def call(body, outs, *args, scratch=(), hbm=0, hbm_out=False):
    memory = [pl.BlockSpec(memory_space=pltpu.HBM if k < hbm else pltpu.VMEM) for k in range(len(args))]
    return pl.pallas_call(
        body, out_shape=outs, in_specs=memory, scratch_shapes=list(scratch),
        out_specs=jax.tree.map(lambda _: pl.BlockSpec(memory_space=pltpu.HBM if hbm_out else pltpu.VMEM), outs),
        compiler_params=pltpu.CompilerParams(vmem_limit_bytes=32 * 2**20),
    )(*args)


def exchange(up, down, axis):
    size = lax.axis_size(axis)
    forward = [(k, (k + 1) % size) for k in range(size)]
    lo = lax.ppermute(up, axis, forward)
    hi = lax.ppermute(down, axis, [(b, a) for a, b in forward])
    return lo, hi


def ahead(value, k):
    size = lax.axis_size("gy")
    return lax.ppermute(value, "gy", [(i, (i + k) % size) for i in range(size)])


def program(pr_in, pi_in, pz_in, px_in, py_in, material, levels):
    parts = lax.axis_size("gy")
    raw = (levels, pr_in, pi_in, px_in, py_in, pz_in, material)
    raw = tuple(pltpu.with_memory_space_constraint(a, pltpu.HBM) for a in raw)
    edge = spec(NZ, TILE, LANES)
    block, tall_block, strip_like = spec(NZ, NX, NY), spec(NZ, RX, LANES), spec(RX, LANES)
    scratch = lambda s, dtype=F32: pltpu.VMEM(s.shape, dtype)
    up, down = call(pack_x, (edge, spec(NZ, 2 * TILE, LANES)), *raw, hbm=7, scratch=[
        pltpu.SMEM((LEVELS,), F32), pltpu.VMEM((5, NZ, TILE, LANES), F32), pltpu.VMEM((5, NZ, TILE, LANES), F32),
        scratch(edge, jnp.int32), scratch(edge, jnp.int32), pltpu.SemaphoreType.DMA((13,))])
    lo, hi = exchange(up, down, "gx")
    pr, pi, ep, trig, own, zup, zdown = call(
        prepare, (block, block, block, spec(6, NZ, NX, NY), spec(6, NX, LANES), spec(8, NX, NY), spec(8, NX, NY)),
        *raw, hbm=7, scratch=[pltpu.SMEM((LEVELS,), F32), scratch(block), scratch(block), scratch(block),
                              scratch(block, jnp.int32), pltpu.SemaphoreType.DMA((7,))])
    zlo, zhi = exchange(zup, zdown, "gz")
    halo, own, up, down = call(
        pack_y, (spec(6, NZ, TILE, LANES), spec(6, RX, LANES), strip_like, spec(2, RX, LANES)), own, lo, hi)
    lo, hi = exchange(up, down, "gy")
    trig_halo, br, bi = call(begin, (spec(6, NZ, TILE, LANES), tall_block, tall_block), pr, pi, ep, trig, halo)
    strip, up, down = call(pack_edges, (spec(6, RX, LANES), spec(17, TILE, LANES), spec(17, TILE, LANES)),
                           trig_halo, halo, own, lo, hi)
    elo, ehi = exchange(up, down, "gz")
    ntrig, cr, ci, some_r, some_i, out = call(
        interior, (spec(6, RX, LANES), tall_block, tall_block, block, block, spec(parts, 2 * NZ - 8, TILE, LANES)),
        br, bi, ep, trig, halo, trig_halo, strip, scratch=[scratch(strip_like)] * 5)
    got = [ahead(out[k], k) for k in EARLY]
    final_r, final_i, out = call(
        boundary, (block, block, spec(parts, 2 * NZ, TILE, LANES)), pr, pi, ep, trig, halo, trig_halo, strip, ntrig, cr, ci,
        some_r, some_i, out, zlo, zhi, elo, ehi, scratch=[pltpu.VMEM((6, RX, LANES), F32)])
    late = {k: ahead(out[k, :8] if k in EARLY else out[k], k) for k in LATE}
    got += [out[0]] + [late[k] for k in range(1, parts)]
    slab = spec(NZ, TILE, parts * LANES)
    circulation, flux = call(finish, (slab, slab), *got, hbm_out=True, scratch=[
        pltpu.VMEM((parts, 8, TILE, LANES), F32), pltpu.VMEM((parts, 2 * NZ - 8, TILE, LANES), F32),
        scratch(slab), scratch(slab), pltpu.SemaphoreType.DMA((8,))])
    return final_r, final_i, circulation, flux


def solution(mesh):
    block = P("gz", "gx", "gy")
    slab = P("gz", ("gx", "gy"), None)
    return jax.shard_map(program, mesh=mesh, in_specs=(block,) * 6 + (P(),),
                         out_specs=(block, block, slab, slab), check_vma=False)
```

```python
import jax
import jax.numpy as jnp
from jax import lax
from jax.experimental import pallas as pl
from jax.experimental.pallas import tpu as pltpu
from jax.sharding import PartitionSpec as P


LEVELS = 8
time_step = 0.15

F32 = jnp.float32
LANES = 128
TILE = 8
NZ, NX, NY = 16, 64, 128
RX = NX + TILE
PR, PI, PX, PY, PZ, EP = range(6)
EARLY = ()
LATE = (4, 2, 6, 3, 5, 1, 7)

SIN = (1.0, -0.16666658222675323, 0.008333050645887852, -0.00019809069635812193, 2.6052216526295524e-06)
COS = (-0.5, 0.0416666604578495, -0.0013888651737943292, 2.4774621124379337e-05, -2.6298400257473986e-07)


def sincos(phase):
    half = phase * 0.5
    u = half * half
    s = SIN[4]
    for k in (3, 2, 1, 0):
        s = s * u + SIN[k]
    s = s * half
    c = COS[4]
    for k in (3, 2, 1, 0):
        c = c * u + COS[k]
    c = c * u + 1.0
    return (c - s) * (c + s), (s + s) * c


def iota(shape, dim):
    return lax.broadcasted_iota(jnp.int32, shape, dim)


def roll(v, shift, axis):
    return pltpu.roll(v, shift % v.shape[axis], axis)


def ahead_x(v):
    return pltpu.roll(v, RX - 1, 0)


def behind_x(v):
    return pltpu.roll(v, 1, 0)


def turned(c, s, r, i):
    return c * r - s * i, c * i + s * r


def turned_back(c, s, r, i):
    return c * r + s * i, c * i - s * r


def row_up(a, row):
    pr, pi, px, py, pz, ep = a
    c, s = sincos(px)
    wr, wi = turned_back(c, s, pr, pi)
    last = row == 6
    pr = jnp.where(last, wr, pr)
    pi = jnp.where(last, wi, pi)
    out = roll(pr, 2, 0)
    out = jnp.where(row >= 2, roll(pi, 4, 0), out)
    out = jnp.where(row == 4, roll(px, 5, 0), out)
    out = jnp.where(row == 5, roll(py, 6, 0), out)
    out = jnp.where(row == 6, roll(pz, 7, 0), out)
    return jnp.where(row == 7, ep, out)


def row_down(a, row):
    pr, pi, px, py, pz, ep = a
    first = jnp.where(row < 3, pr, jnp.where(row < 6, roll(pi, 3, 0), roll(px, 6, 0)))
    second = jnp.where(row < 2, py, jnp.where(row < 4, roll(pz, 2, 0), roll(ep, 4, 0)))
    return first, second


def scaled_levels(levels):
    return [1.0 + time_step * (levels[k] - 6.0) for k in range(LEVELS)]


def material_gain(m, values):
    e = jnp.full(m.shape, values[LEVELS - 1], F32)
    for k in range(LEVELS - 1):
        e = jnp.where(m == k, values[k], e)
    return e


def start_copies(pairs, sems):
    copies = [pltpu.make_async_copy(a, b, sems.at[n]) for n, (a, b) in enumerate(pairs)]
    for copy in copies:
        copy.start()
    return copies


def pack_first(levels_in, pr, pi, px, py, pz, mat, up, down, zup, zdown,
               levels, top, low, top_mat, low_mat, far, end_mat, sems):
    fields = (pr, pi, px, py, pz)
    pairs = [(levels_in, levels)]
    pairs += [(q.at[:, pl.ds(NX - TILE, TILE), :], top.at[k]) for k, q in enumerate(fields)]
    pairs += [(q.at[:, pl.ds(0, TILE), :], low.at[k]) for k, q in enumerate(fields)]
    pairs += [(mat.at[:, pl.ds(NX - TILE, TILE), :], top_mat), (mat.at[:, pl.ds(0, TILE), :], low_mat)]
    ready = len(pairs)
    pairs += [(q.at[14], far.at[k]) for k, q in enumerate((pr, pi, pz))]
    pairs += [(mat.at[0], end_mat.at[0]), (mat.at[15], end_mat.at[1])]
    pairs += [(q.at[15], zup.at[2 + k]) for k, q in enumerate(fields)]
    pairs += [(q.at[0], zdown.at[2 + k]) for k, q in enumerate(fields)]
    pairs += [(pr.at[1], zdown.at[0]), (pi.at[1], zdown.at[1])]
    copies = start_copies(pairs, sems)
    for copy in copies[:ready]:
        copy.wait()
    row = iota((TILE, LANES), 0)
    values = scaled_levels(levels)

    def body(z, carry):
        up[z] = row_up([top[k, z] for k in range(5)] + [material_gain(top_mat[z], values)], row)
        first, second = row_down([low[k, z] for k in range(5)] + [material_gain(low_mat[z], values)], row)
        down[z, :TILE, :] = first
        down[z, TILE:, :] = second
        return carry

    lax.fori_loop(0, NZ, body, 0, unroll=4)
    for copy in copies[ready:]:
        copy.wait()
    c, s = sincos(far[2])
    zup[0], zup[1] = turned_back(c, s, far[0], far[1])
    zdown[7] = material_gain(end_mat[0], values)
    zup[7] = material_gain(end_mat[1], values)


def prepare(levels_in, pr_in, pi_in, px_in, py_in, pz_in, mat_in, pr, pi, ep, trig, own,
            levels, px, py, pz, mat, sems):
    pairs = [(levels_in, levels), (mat_in, mat), (pz_in, pz), (px_in, px), (py_in, py), (pr_in, pr), (pi_in, pi)]
    copies = start_copies(pairs, sems)
    copies[0].wait()
    copies[1].wait()
    values = scaled_levels(levels)

    def gains(z, carry):
        ep[z] = material_gain(mat[z], values)
        return carry

    lax.fori_loop(0, NZ, gains, 0)
    for n, q in enumerate((pz, px, py)):
        copies[2 + n].wait()

        def angles(z, carry):
            trig[2 * n, z], trig[2 * n + 1, z] = sincos(q[z])
            return carry

        lax.fori_loop(0, NZ, angles, 0)
    copies[5].wait()
    copies[6].wait()
    group = iota((TILE, LANES), 1) // 8

    def columns(t, carry):
        rows = pl.ds(pl.multiple_of(t * TILE, TILE), TILE)
        for k, q in enumerate((pr, pi, px, py, pz, ep)):
            acc = roll(q[0, rows, :], -126, 1)
            for z in range(1, NZ):
                acc = jnp.where(group == z, roll(q[z, rows, :], 8 * z - 126, 1), acc)
            own[k, rows, :] = acc
        return carry

    lax.fori_loop(0, NX // TILE, columns, 0)


def pack_y(own_in, lo, hi, halo, own, up, down):
    row = iota((TILE, LANES), 0)
    gx = lax.axis_index("gx")
    keep = jnp.where(row < 4, jnp.where(gx < lax.axis_size("gx") - 1, 1, 0), jnp.where(gx > 0, 1, 0)) > 0
    low_rows = row >= 6
    last = row == 7
    group = iota((TILE, LANES), 1) // 8
    acc = [jnp.zeros((TILE, LANES), F32) for _ in range(6)]
    for z in range(NZ):
        l = lo[z]
        a = hi[z, :TILE, :]
        b = hi[z, TILE:, :]
        zero = jnp.zeros_like(l)
        tiles = (
            jnp.where(keep, jnp.where(low_rows, roll(l, 6, 0), a), zero),
            jnp.where(keep, jnp.where(low_rows, roll(l, 4, 0), roll(a, -3, 0)), zero),
            jnp.where(last, roll(l, 3, 0), jnp.where(row < 2, roll(a, -6, 0), zero)),
            jnp.where(last, roll(l, 2, 0), jnp.where(row < 2, b, zero)),
            jnp.where(last, roll(l, 1, 0), jnp.where(row < 2, roll(b, -2, 0), zero)),
            jnp.where(last, l, jnp.where(row < 2, roll(b, -4, 0), zero)),
        )
        for k, tile in enumerate(tiles):
            halo[k, z] = tile
            acc[k] = jnp.where(group == z, roll(tile, 8 * z - 126, 1), acc[k])
    columns = []
    for k in range(6):
        v = jnp.concatenate([own_in[k], acc[k]], axis=0)
        own[k] = v
        columns.append(v)
    slot = iota((RX, LANES), 1) % 8
    vr, vi, vx, vy, vz, ve = columns
    c, s = sincos(vy)
    wr, wi = turned_back(c, s, vr, vi)
    ur = jnp.where(slot == 0, wr, vr)
    ui = jnp.where(slot == 0, wi, vi)
    out = jnp.where(slot < 2, ur, roll(ui, 2, 1))
    out = jnp.where(slot == 4, roll(vx, 3, 1), out)
    out = jnp.where(slot == 5, roll(vy, 4, 1), out)
    out = jnp.where(slot == 6, roll(vz, 5, 1), out)
    out = jnp.where(slot == 7, roll(ve, 6, 1), out)
    up[...] = out
    down[0] = jnp.where(slot < 3, roll(vr, -2, 1), jnp.where(slot < 6, roll(vi, 1, 1), roll(vx, 4, 1)))
    down[1] = jnp.where(slot < 2, roll(vy, -2, 1), jnp.where(slot < 4, vz, roll(ve, 2, 1)))


def tall(q, h, z):
    return jnp.concatenate([q[z], h[z]], axis=0)


def angles_at(trig, trig_halo, n, z):
    return jnp.concatenate([trig[n, z], trig_halo[n, z]], axis=0)


def advance(centre, above, below_turned, trig, edge, gain, lane):
    r, i = centre
    cz, sz, cx, sx, cy, sy = trig
    t = turned(cx, sx, ahead_x(r), ahead_x(i))
    w = turned_back(cx, sx, r, i)
    sum_r, sum_i = t[0] + behind_x(w[0]), t[1] + behind_x(w[1])
    if below_turned is not None:
        sum_r, sum_i = sum_r + below_turned[0], sum_i + below_turned[1]
    if above is not None:
        t = turned(cz, sz, *above)
        sum_r, sum_i = sum_r + t[0], sum_i + t[1]
    wr, wi = turned_back(cy, sy, r, i)
    fr, fi, wr, wi = roll(r, -1, 1), roll(i, -1, 1), roll(wr, 1, 1), roll(wi, 1, 1)
    if edge is not None:
        fr, fi = jnp.where(lane == 127, edge[0], fr), jnp.where(lane == 127, edge[1], fi)
        wr, wi = jnp.where(lane == 0, edge[0], wr), jnp.where(lane == 0, edge[1], wi)
    t = turned(cy, sy, fr, fi)
    sum_r, sum_i = sum_r + t[0] + wr, sum_i + t[1] + wi
    gain = gain - time_step * (r * r + i * i)
    return gain * r + time_step * sum_r, gain * i + time_step * sum_i


def begin(pr, pi, ep, trig, halo, trig_halo, br, bi):
    lane = iota((RX, LANES), 1)
    zero = jnp.zeros((RX, LANES), F32)

    def angles(z, carry):
        for n, k in enumerate((PZ, PX, PY)):
            trig_halo[2 * n, z], trig_halo[2 * n + 1, z] = sincos(halo[k, z])
        return carry

    lax.fori_loop(0, NZ, angles, 0)
    none = (zero, zero)

    def layer(z):
        return tall(pr, halo.at[PR], z), tall(pi, halo.at[PI], z)

    def one(z, above, below):
        t = [angles_at(trig, trig_halo, n, z) for n in range(6)]
        if below is not None:
            below = turned_back(angles_at(trig, trig_halo, 0, below), angles_at(trig, trig_halo, 1, below),
                                *layer(below))
        if above is not None:
            above = layer(above)
        br[z], bi[z] = advance(layer(z), above, below, t, none, tall(ep, halo.at[EP], z), lane)

    one(0, 1, None)

    def body(z, carry):
        one(z, z + 1, z - 1)
        return carry

    lax.fori_loop(1, NZ - 1, body, 0)
    one(NZ - 1, None, NZ - 2)


def pack_edges(trig_halo, halo, own, lo, hi, strip, up, down):
    lane = iota((RX, LANES), 1)
    slot = lane % 8
    group = lane // 8
    gy = lax.axis_index("gy")
    keep = jnp.where((slot >= 2) & (slot < 5), jnp.where(gy < lax.axis_size("gy") - 1, 1, 0),
                     jnp.where((slot >= 5) & (slot < 7), jnp.where(gy > 0, 1, 0), 1)) > 0
    l = lo[...]
    a = hi[0]
    b = hi[1]
    zero = jnp.zeros_like(l)

    def join(k, from_hi, from_lo):
        v = own[k]
        out = jnp.where(slot < 2, v, roll(v, 5, 1))
        out = jnp.where((slot >= 2) & (slot < 5), from_hi, out)
        return jnp.where((slot == 5) | (slot == 6), from_lo, out)

    one = slot == 6
    strip[PR] = jnp.where(keep, join(PR, roll(a, 2, 1), roll(l, 5, 1)), zero)
    strip[PI] = jnp.where(keep, join(PI, roll(a, -1, 1), roll(l, 3, 1)), zero)
    strip[PX] = join(PX, roll(a, -4, 1), jnp.where(one, roll(l, 2, 1), zero))
    strip[PY] = join(PY, roll(b, 2, 1), jnp.where(one, roll(l, 1, 1), zero))
    strip[PZ] = join(PZ, b, jnp.where(one, l, zero))
    strip[EP] = join(EP, roll(b, -2, 1), jnp.where(one, roll(l, -1, 1), zero))
    up[0], up[1] = turned_back(trig_halo[0, 14], trig_halo[1, 14], halo[PR, 14], halo[PI, 14])
    down[0] = halo[PR, 1]
    down[1] = halo[PI, 1]
    for k in range(6):
        up[2 + k] = halo[k, 15]
        down[2 + k] = halo[k, 0]
    c, s = sincos(strip[PZ])
    wr, wi = turned_back(c, s, strip[PR], strip[PI])
    out = jnp.where(group == 0, roll(wr, -8 * 14, 1), roll(wi, -8 * 13, 1))
    for k in range(6):
        out = jnp.where(group == 2 + k, roll(strip[k], 8 * (2 + k - 15), 1), out)
    for t in range(RX // TILE):
        up[8 + t] = out[t * TILE:(t + 1) * TILE]
    out = jnp.where(group == 0, roll(strip[PR], -8, 1), strip[PI])
    for k in range(6):
        out = jnp.where(group == 2 + k, roll(strip[k], 8 * (2 + k), 1), out)
    for t in range(RX // TILE):
        down[8 + t] = out[t * TILE:(t + 1) * TILE]


def shift_of(group):
    return (125 - 8 * group) % 128


def on(test):
    return jnp.where(test, 1, 0)


def inside_masks():
    row = iota((RX, LANES), 0)
    slot = iota((RX, LANES), 1) % 8
    gx, gy = lax.axis_index("gx"), lax.axis_index("gy")
    keep_x = jnp.where(row < NX, 1, jnp.where(row < NX + 4, on(gx < lax.axis_size("gx") - 1), on(gx > 0)))
    keep_y = jnp.where((slot >= 2) & (slot < 5), on(gy < lax.axis_size("gy") - 1),
                       jnp.where((slot >= 5) & (slot < 7), on(gy > 0), 1))
    return keep_x, keep_x * keep_y


def edge_columns(slot, ntrig, r, i):
    wr, wi = turned_back(ntrig[4], ntrig[5], r, i)
    return jnp.where(slot == 3, roll(wr, -3, 1), r), jnp.where(slot == 3, roll(wi, -3, 1), i)


def masked_rows(v, keep_tile):
    return jnp.concatenate([v[:NX], jnp.where(keep_tile > 0, v[NX:], 0.0)], axis=0)


def analyse(z, r, i, trig_x, trig_y, columns, jx_column, lane, rows, out, spot):
    shift = shift_of(z)
    own_r, own_i = r[:NX], i[:NX]
    t = turned(trig_x[0][:NX], trig_x[1][:NX], ahead_x(r)[:NX], ahead_x(i)[:NX])
    jx = own_r * t[1] - own_i * t[0]
    last = lane == 127
    fr = jnp.where(last, roll_by(columns[0], shift), roll(r, -1, 1))
    fi = jnp.where(last, roll_by(columns[1], shift), roll(i, -1, 1))
    t = turned(*trig_y, fr, fi)
    jy = r * t[1] - i * t[0]
    jx_next = jnp.where(last[:NX], roll_by(jx_column[:NX], shift), roll(jx, -1, 1))
    circulation = jx + ahead_x(jy)[:NX] - jx_next - jy[:NX]
    rows[pl.ds(spot * NX, NX), :] = jx
    for j in range(NX // TILE):
        away = (j + out.shape[0] - lax.axis_index("gy")) % out.shape[0]
        out[away, spot] = circulation[j * TILE:(j + 1) * TILE]


def prefix(rows, out, spots, gap):
    triangle = triangle_of().astype(jnp.bfloat16)
    v = rows[spots.start * NX:spots.stop * NX, :]
    a = v.astype(jnp.bfloat16)
    v = v - a.astype(F32)
    b = v.astype(jnp.bfloat16)
    c = (v - b.astype(F32)).astype(jnp.bfloat16)
    sums = jnp.dot(jnp.concatenate([c, b, a], axis=0), triangle, preferred_element_type=F32)
    n = a.shape[0]
    sums = sums[:n] + sums[n:2 * n] + sums[2 * n:]
    for k, spot in enumerate(spots):
        for j in range(NX // TILE):
            away = (j + out.shape[0] - lax.axis_index("gy")) % out.shape[0]
            out[away, gap + spot] = sums[k * NX + j * TILE:k * NX + (j + 1) * TILE]


def roll_by(v, shift):
    return pltpu.roll(v, shift, 1)


def triangle_of():
    return jnp.where(iota((LANES, LANES), 0) <= iota((LANES, LANES), 1), 1.0, 0.0).astype(F32)


def interior(pr_in, pi_in, ep, trig, halo, trig_halo, strip, ntrig, cr, ci, final_r, final_i, out,
             er, ei, nr, ni, jx_edge, rows):
    lane = iota((RX, LANES), 1)
    slot = lane % 8
    keep_x, keep_xy = inside_masks()
    keep_tile = keep_x[NX:]
    zero = jnp.zeros((RX, LANES), F32)
    for n, k in enumerate((PZ, PX, PY)):
        ntrig[2 * n], ntrig[2 * n + 1] = sincos(strip[k])
    nt = lambda: [ntrig[n] for n in range(6)]
    er[...], ei[...] = edge_columns(slot, ntrig, strip[PR], strip[PI])

    def fix(z, carry):
        shift = shift_of(z)
        xr, xi = roll_by(er[...], shift), roll_by(ei[...], shift)
        cy = jnp.where(lane == 127, angles_at(trig, trig_halo, 4, z), jnp.where(lane == 0, 1.0, 0.0)) * time_step
        sy = jnp.where(lane == 127, angles_at(trig, trig_halo, 5, z), 0.0) * time_step
        hr, hi = turned(cy, sy, xr, xi)
        cr[z] = masked_rows(pr_in[z] + hr, keep_tile)
        ci[z] = masked_rows(pi_in[z] + hi, keep_tile)
        return carry

    for z in range(NZ):
        fix(z, 0)

    def strips(r, i):
        w = turned_back(ntrig[0], ntrig[1], r, i)
        v = advance((r, i), (roll(r, -8, 1), roll(i, -8, 1)), (roll(w[0], 8, 1), roll(w[1], 8, 1)), nt(), None,
                    strip[EP], lane)
        return jnp.where(keep_xy > 0, v[0], zero), jnp.where(keep_xy > 0, v[1], zero)

    mr, mi = strips(strip[PR], strip[PI])
    er[...], ei[...] = edge_columns(slot, ntrig, mr, mi)
    r, i = strips(mr, mi)
    nr[...] = r
    ni[...] = i
    t = turned(ntrig[2], ntrig[3], ahead_x(r), ahead_x(i))
    jx_edge[...] = r * t[1] - i * t[0]

    def second(z, carry):
        last_layer(z, (cr[z], ci[z]), (cr[z + 1], ci[z + 1]), (cr[z - 1], ci[z - 1]), ep, trig, halo, trig_halo,
                   (er[...], ei[...]), (nr[...], ni[...]), jx_edge[...], keep_x, lane, rows,
                   final_r, final_i, out, None, z - 2)
        return carry

    for z in range(2, NZ - 2):
        second(z, 0)
        if z % 4 == 1:
            prefix(rows, out, range(z - 5, z - 1), NZ - 4)


def last_layer(z, centre, above, below, ep, trig, halo, trig_halo, edges, columns, jx_column, keep_x, lane,
               rows, final_r, final_i, out, below_turned, spot):
    t = [angles_at(trig, trig_halo, n, z) for n in range(6)]
    if below_turned is None:
        below_turned = turned_back(angles_at(trig, trig_halo, 0, z - 1), angles_at(trig, trig_halo, 1, z - 1), *below)
    shift = shift_of(z)
    edge = roll_by(edges[0], shift), roll_by(edges[1], shift)
    r, i = advance(centre, above, below_turned, t, edge, tall(ep, halo.at[EP], z), lane)
    r = masked_rows(r, keep_x[NX:])
    i = masked_rows(i, keep_x[NX:])
    final_r[spot] = r[:NX]
    final_i[spot] = i[:NX]
    analyse(z, r, i, t[2:4], t[4:6], columns, jx_column, lane, rows, out, spot)


def boundary(pr, pi, ep, trig, halo, trig_halo, strip, ntrig0, cr, ci, middle_out,
             zlo, zhi, elo, ehi, final_r, final_i, out, ntrig1, rows):
    lane = iota((RX, LANES), 1)
    slot = lane % 8
    group = lane // 8
    keep_x, keep_xy = inside_masks()
    gz = lax.axis_index("gz")
    z_hi, z_lo = on(gz < lax.axis_size("gz") - 1), on(gz > 0)
    keep_z = jnp.where(group < 8, z_hi, z_lo)
    zero = jnp.zeros((RX, LANES), F32)
    for away in range(out.shape[0]):
        out[away, 8:] = middle_out[away]
    lo8 = jnp.concatenate([elo[8 + t] for t in range(RX // TILE)], axis=0)
    hi8 = jnp.concatenate([ehi[8 + t] for t in range(RX // TILE)], axis=0)

    def beyond(k, outer):
        v = jnp.where(group == 0, roll(hi8, -8 * (2 + k), 1), roll(lo8, 8 * (15 - 2 - k), 1))
        if outer is not None:
            v = jnp.where(group == 1, roll(hi8, 8 * (1 - outer), 1), v)
            v = jnp.where(group == 14, roll(lo8, 8 * (14 - outer), 1), v)
        return v

    for n, k in enumerate((PZ, PX, PY)):
        v = beyond(k, None)
        if k == PZ:
            v = jnp.where(group == 14, zero, v)
        ntrig1[2 * n], ntrig1[2 * n + 1] = sincos(v)
    trigs = (ntrig0, ntrig1)
    gains = (strip[EP], beyond(EP, None))

    def step_strips(halves, wanted):
        w = [turned_back(trigs[h][0], trigs[h][1], *halves[h]) for h in range(2)]
        results = []
        for h in wanted:
            g = 1 - h
            below = [jnp.where(group == 0, roll(w[g][n], 8, 1), roll(w[h][n], 8, 1)) for n in range(2)]
            above = [jnp.where(group == 15, roll(halves[g][n], -8, 1), roll(halves[h][n], -8, 1)) for n in range(2)]
            v = advance(halves[h], above, below, [trigs[h][n] for n in range(6)], None, gains[h], lane)
            keep = keep_xy if h == 0 else keep_xy * keep_z
            results.append([jnp.where(keep > 0, u, zero) for u in v])
        return results

    halves = ((strip[PR], strip[PI]),
              (jnp.where(keep_z > 0, beyond(PR, 0), zero), jnp.where(keep_z > 0, beyond(PI, 1), zero)))
    beyond_edge = edge_columns(slot, ntrig1, *halves[1])
    middle = step_strips(halves, (0, 1))
    edges = edge_columns(slot, ntrig0, *middle[0])
    (columns,) = step_strips(middle, (0,))
    t = turned(ntrig0[2], ntrig0[3], ahead_x(columns[0]), ahead_x(columns[1]))
    jx_column = columns[0] * t[1] - columns[1] * t[0]

    ok_lo = jnp.broadcast_to(z_lo, (RX, LANES)) > 0
    ok_hi = jnp.broadcast_to(z_hi, (RX, LANES)) > 0

    def got(main, tiles, n):
        return jnp.concatenate([main[n], tiles[n]], axis=0)

    def angles(main, tiles):
        found = []
        for k in (PZ, PX, PY):
            found += list(sincos(got(main, tiles, 2 + k)))
        return found

    def own(z):
        return tall(pr, halo.at[PR], z), tall(pi, halo.at[PI], z)

    def masked(ok, v):
        return tuple(jnp.where(ok, u, zero) for u in v)

    def at(z, n):
        return angles_at(trig, trig_halo, n, z)

    t_lo = angles(zlo, elo)
    outer = masked(ok_lo, (got(zlo, elo, 0), got(zlo, elo, 1)))
    inner = masked(ok_lo, (got(zlo, elo, 2), got(zlo, elo, 3)))
    edge = roll_by(beyond_edge[0], shift_of(15)), roll_by(beyond_edge[1], shift_of(15))
    v = masked(ok_lo & (keep_x > 0), advance(inner, own(0), outer, t_lo, edge, got(zlo, elo, 2 + EP), lane))
    w = turned_back(t_lo[0], t_lo[1], *inner)
    first = masked(keep_x > 0, (cr[0] + time_step * w[0], ci[0] + time_step * w[1]))
    below = turned_back(t_lo[0], t_lo[1], *v)
    common = (ep, trig, halo, trig_halo, edges, columns, jx_column, keep_x, lane, rows, final_r, final_i, out)
    last_layer(0, first, (cr[1], ci[1]), None, *common, below, 0)
    last_layer(1, (cr[1], ci[1]), (cr[2], ci[2]), first, *common, None, 1)
    t_hi = angles(zhi, ehi)
    outer = masked(ok_hi, (got(zhi, ehi, 0), got(zhi, ehi, 1)))
    inner = masked(ok_hi, (got(zhi, ehi, 2), got(zhi, ehi, 3)))
    edge = roll_by(beyond_edge[0], shift_of(0)), roll_by(beyond_edge[1], shift_of(0))
    below = turned_back(at(15, 0), at(15, 1), *own(15))
    v = masked(ok_hi & (keep_x > 0), advance(inner, outer, below, t_hi, edge, got(zhi, ehi, 2 + EP), lane))
    w = turned(at(15, 0), at(15, 1), *inner)
    final = masked(keep_x > 0, (cr[15] + time_step * w[0], ci[15] + time_step * w[1]))
    last_layer(14, (cr[14], ci[14]), final, (cr[13], ci[13]), *common, None, 2)
    last_layer(15, final, v, (cr[14], ci[14]), *common, None, 3)
    prefix(rows, out, range(4), 4)


def store(some_r, some_i, ends_r, ends_i, final_r, final_i, sems):
    pairs = []
    for some, ends, final in ((some_r, ends_r, final_r), (some_i, ends_i, final_i)):
        pairs += [(some, final.at[pl.ds(2, NZ - 4)]), (ends.at[pl.ds(0, 2)], final.at[pl.ds(0, 2)]),
                  (ends.at[pl.ds(2, 2)], final.at[pl.ds(NZ - 2, 2)])]
    for copy in start_copies(pairs, sems):
        copy.wait()


ENDS = (0, 1, NZ - 2, NZ - 1)


def finish(*refs):
    parts = lax.axis_size("gy")
    got, (circulation, flux, ends, middle, full_c, full_f, sems) = refs[:-7], refs[-7:]
    me = lax.axis_index("gy")
    for k in range(parts):
        source = (me + parts - k) % parts
        if k in EARLY:
            ends[source] = got[len(EARLY) + k][...]
            middle[source] = got[EARLY.index(k)][...]
        else:
            ends[source] = got[len(EARLY) + k][:8]
            middle[source] = got[len(EARLY) + k][8:]

    def layer(pieces, spot, gap, z):
        before = jnp.zeros((TILE, 1), F32)
        for j in range(parts):
            full_c[z, :, j * LANES:(j + 1) * LANES] = pieces[j, spot]
            v = pieces[j, spot + gap]
            full_f[z, :, j * LANES:(j + 1) * LANES] = v + before
            before = before + v[:, LANES - 1:]

    copies = []

    def send(first):
        for a, b in ((full_c, circulation), (full_f, flux)):
            copies.append(pltpu.make_async_copy(a.at[pl.ds(first, 4)], b.at[pl.ds(first, 4)], sems.at[len(copies)]))
            copies[-1].start()

    for first in (4, 8, 0, 12):
        for z in range(first, first + 4):
            if z in ENDS:
                layer(ends, ENDS.index(z), 4, z)
            else:
                layer(middle, z - 2, NZ - 4, z)
        send(first)
    for copy in copies:
        copy.wait()


def spec(*shape):
    return jax.ShapeDtypeStruct(shape, F32)


def call(body, outs, *args, scratch=(), hbm=0, hbm_out=False):
    memory = [pl.BlockSpec(memory_space=pltpu.HBM if k < hbm else pltpu.VMEM) for k in range(len(args))]
    return pl.pallas_call(
        body, out_shape=outs, in_specs=memory, scratch_shapes=list(scratch),
        out_specs=jax.tree.map(lambda _: pl.BlockSpec(memory_space=pltpu.HBM if hbm_out else pltpu.VMEM), outs),
        compiler_params=pltpu.CompilerParams(vmem_limit_bytes=32 * 2**20),
    )(*args)


def exchange(up, down, axis):
    size = lax.axis_size(axis)
    forward = [(k, (k + 1) % size) for k in range(size)]
    lo = lax.ppermute(up, axis, forward)
    hi = lax.ppermute(down, axis, [(b, a) for a, b in forward])
    return lo, hi


def ahead(value, k):
    size = lax.axis_size("gy")
    return lax.ppermute(value, "gy", [(i, (i + k) % size) for i in range(size)])


def program(pr_in, pi_in, pz_in, px_in, py_in, material, levels):
    parts = lax.axis_size("gy")
    raw = (levels, pr_in, pi_in, px_in, py_in, pz_in, material)
    raw = tuple(pltpu.with_memory_space_constraint(a, pltpu.HBM) for a in raw)
    edge = spec(NZ, TILE, LANES)
    block, tall_block, strip_like = spec(NZ, NX, NY), spec(NZ, RX, LANES), spec(RX, LANES)
    scratch = lambda s, dtype=F32: pltpu.VMEM(s.shape, dtype)
    layers = spec(8, NX, NY)
    up, down, zup, zdown = call(pack_first, (edge, spec(NZ, 2 * TILE, LANES), layers, layers), *raw, hbm=7, scratch=[
        pltpu.SMEM((LEVELS,), F32), pltpu.VMEM((5, NZ, TILE, LANES), F32), pltpu.VMEM((5, NZ, TILE, LANES), F32),
        scratch(edge, jnp.int32), scratch(edge, jnp.int32), pltpu.VMEM((3, NX, NY), F32),
        pltpu.VMEM((2, NX, NY), jnp.int32), pltpu.SemaphoreType.DMA((30,))])
    lo, hi = exchange(up, down, "gx")
    zlo, zhi = exchange(zup, zdown, "gz")
    pr, pi, ep, trig, own = call(
        prepare, (block, block, block, spec(6, NZ, NX, NY), spec(6, NX, LANES)),
        *raw, hbm=7, scratch=[pltpu.SMEM((LEVELS,), F32), scratch(block), scratch(block), scratch(block),
                              scratch(block, jnp.int32), pltpu.SemaphoreType.DMA((7,))])
    halo, own, up, down = call(
        pack_y, (spec(6, NZ, TILE, LANES), spec(6, RX, LANES), strip_like, spec(2, RX, LANES)), own, lo, hi)
    lo, hi = exchange(up, down, "gy")
    trig_halo, br, bi = call(begin, (spec(6, NZ, TILE, LANES), tall_block, tall_block), pr, pi, ep, trig, halo)
    strip, up, down = call(pack_edges, (spec(6, RX, LANES), spec(17, TILE, LANES), spec(17, TILE, LANES)),
                           trig_halo, halo, own, lo, hi)
    elo, ehi = exchange(up, down, "gz")
    middle_block, ends_block = spec(NZ - 4, NX, NY), spec(4, NX, NY)
    ntrig, cr, ci, some_r, some_i, out = call(
        interior, (spec(6, RX, LANES), tall_block, tall_block, middle_block, middle_block,
                   spec(parts, 2 * NZ - 8, TILE, LANES)),
        br, bi, ep, trig, halo, trig_halo, strip,
        scratch=[scratch(strip_like)] * 5 + [pltpu.VMEM(((NZ - 4) * NX, NY), F32)])
    got = [ahead(out[k], k) for k in EARLY]
    ends_r, ends_i, out = call(
        boundary, (ends_block, ends_block, spec(parts, 2 * NZ, TILE, LANES)), pr, pi, ep, trig, halo, trig_halo, strip,
        ntrig, cr, ci, out, zlo, zhi, elo, ehi,
        scratch=[pltpu.VMEM((6, RX, LANES), F32), pltpu.VMEM((4 * NX, NY), F32)])
    late = {k: ahead(out[k, :8] if k in EARLY else out[k], k) for k in LATE}
    final_r, final_i = call(store, (block, block), some_r, some_i, ends_r, ends_i, hbm_out=True,
                            scratch=[pltpu.SemaphoreType.DMA((6,))])
    got += [out[0]] + [late[k] for k in range(1, parts)]
    slab = spec(NZ, TILE, parts * LANES)
    circulation, flux = call(finish, (slab, slab), *got, hbm_out=True, scratch=[
        pltpu.VMEM((parts, 8, TILE, LANES), F32), pltpu.VMEM((parts, 2 * NZ - 8, TILE, LANES), F32),
        scratch(slab), scratch(slab), pltpu.SemaphoreType.DMA((8,))])
    return final_r, final_i, circulation, flux


def solution(mesh):
    block = P("gz", "gx", "gy")
    slab = P("gz", ("gx", "gy"), None)
    return jax.shard_map(program, mesh=mesh, in_specs=(block,) * 6 + (P(),),
                         out_specs=(block, block, slab, slab), check_vma=False)
```

```python
import jax
import jax.numpy as jnp
from jax import lax
from jax.experimental import pallas as pl
from jax.experimental.pallas import tpu as pltpu
from jax.sharding import PartitionSpec as P


LEVELS = 8
time_step = 0.15

F32 = jnp.float32
LANES = 128
TILE = 8
NZ, NX, NY = 16, 64, 128
RX = NX + TILE
PR, PI, PX, PY, PZ, EP = range(6)
EARLY = ()
LATE = (4, 2, 6, 3, 5, 1, 7)

SIN = (1.0, -0.16666658222675323, 0.008333050645887852, -0.00019809069635812193, 2.6052216526295524e-06)
COS = (-0.5, 0.0416666604578495, -0.0013888651737943292, 2.4774621124379337e-05, -2.6298400257473986e-07)


def sincos(phase):
    half = phase * 0.5
    u = half * half
    s = SIN[4]
    for k in (3, 2, 1, 0):
        s = s * u + SIN[k]
    s = s * half
    c = COS[4]
    for k in (3, 2, 1, 0):
        c = c * u + COS[k]
    c = c * u + 1.0
    return (c - s) * (c + s), (s + s) * c


def iota(shape, dim):
    return lax.broadcasted_iota(jnp.int32, shape, dim)


def roll(v, shift, axis):
    return pltpu.roll(v, shift % v.shape[axis], axis)


def ahead_x(v):
    return pltpu.roll(v, RX - 1, 0)


def behind_x(v):
    return pltpu.roll(v, 1, 0)


def turned(c, s, r, i):
    return c * r - s * i, c * i + s * r


def turned_back(c, s, r, i):
    return c * r + s * i, c * i - s * r


def scaled_levels(levels):
    return [1.0 + time_step * (levels[k] - 6.0) for k in range(LEVELS)]


def material_gain(m, values):
    e = jnp.full(m.shape, values[LEVELS - 1], F32)
    for k in range(LEVELS - 1):
        e = jnp.where(m == k, values[k], e)
    return e


def start_copies(pairs, sems):
    copies = [pltpu.make_async_copy(a, b, sems.at[n]) for n, (a, b) in enumerate(pairs)]
    for copy in copies:
        copy.start()
    return copies


def pack_first(levels_in, pr, pi, px, py, pz, mat, up, down, zup, zdown,
               levels, outer, row_mat, far, sems):
    fields = (pr, pi, px, py, pz)
    pairs = [(levels_in, levels)]
    pairs += [(q.at[:, NX - 2, :], outer.at[k]) for k, q in enumerate((pr, pi, px))]
    pairs += [(mat.at[:, row, :], row_mat.at[k]) for k, row in enumerate((0, 1, NX - 1))]
    pairs += [(q.at[:, NX - 1, :], up.at[2 + k]) for k, q in enumerate(fields)]
    pairs += [(q.at[:, row, :], down.at[3 * k + row]) for k, q in enumerate((pr, pi)) for row in range(3)]
    pairs += [(q.at[:, row, :], down.at[6 + 2 * k + row]) for k, q in enumerate((px, py, pz)) for row in range(2)]
    pairs += [(q.at[NZ - 1], far.at[k]) for k, q in enumerate((pr, pi, pz))]
    pairs += [(pr.at[0], zdown.at[0]), (pi.at[0], zdown.at[1])]
    for copy in start_copies(pairs, sems):
        copy.wait()
    values = scaled_levels(levels)
    c, s = sincos(outer[2])
    up[0], up[1] = turned_back(c, s, outer[0], outer[1])
    up[7] = material_gain(row_mat[2], values)
    down[12] = material_gain(row_mat[0], values)
    down[13] = material_gain(row_mat[1], values)
    c, s = sincos(far[2])
    zup[0], zup[1] = turned_back(c, s, far[0], far[1])


def columns(levels, pr, pi, px, py, pz, mat, own):
    group = iota((TILE, LANES), 1) // 8
    values = scaled_levels(levels)
    for k, q in enumerate((pr, pi, px, py, pz, mat)):
        for t in range(NX // TILE):
            rows = slice(t * TILE, (t + 1) * TILE)
            acc = roll(q[0, rows, :], -126, 1)
            for z in range(1, NZ):
                acc = jnp.where(group == z, roll(q[z, rows, :], 8 * z - 126, 1), acc)
            own[k, rows, :] = material_gain(acc, values) if k == EP else acc


def angles(levels, px, py, pz, mat, ep, trig):
    values = scaled_levels(levels)

    def body(z, carry):
        ep[z] = material_gain(mat[z], values)
        for n, q in enumerate((pz, px, py)):
            trig[2 * n, z], trig[2 * n + 1, z] = sincos(q[z])
        return carry

    lax.fori_loop(0, NZ, body, 0)


def pack_y(own_in, lo, hi, halo, own, up, down):
    row = iota((TILE, LANES), 0)
    gx = lax.axis_index("gx")
    keep = jnp.where(row < 4, jnp.where(gx < lax.axis_size("gx") - 1, 1, 0), jnp.where(gx > 0, 1, 0)) > 0
    group = iota((TILE, LANES), 1) // 8
    acc = [jnp.zeros((TILE, LANES), F32) for _ in range(6)]
    zero = jnp.zeros((TILE, LANES), F32)

    def rows_at(z, placed):
        out = zero
        for at, (ref, k) in placed.items():
            out = jnp.where(row == at, jnp.broadcast_to(ref[k, z:z + 1, :], (TILE, LANES)), out)
        return out

    for z in range(NZ):
        tiles = [jnp.where(keep, rows_at(z, {0: (hi, 3 * k), 1: (hi, 3 * k + 1), 2: (hi, 3 * k + 2),
                                             6: (lo, k), 7: (lo, 2 + k)}), zero) for k in range(2)]
        tiles += [rows_at(z, {0: (hi, 6 + 2 * k), 1: (hi, 7 + 2 * k), 7: (lo, 4 + k)}) for k in range(4)]
        for k, tile in enumerate(tiles):
            halo[k, z] = tile
            acc[k] = jnp.where(group == z, roll(tile, 8 * z - 126, 1), acc[k])
    columns = []
    for k in range(6):
        v = jnp.concatenate([own_in[k], acc[k]], axis=0)
        own[k] = v
        columns.append(v)
    slot = iota((RX, LANES), 1) % 8
    vr, vi, vx, vy, vz, ve = columns
    c, s = sincos(vy)
    wr, wi = turned_back(c, s, vr, vi)
    ur = jnp.where(slot == 0, wr, vr)
    ui = jnp.where(slot == 0, wi, vi)
    out = jnp.where(slot < 2, ur, roll(ui, 2, 1))
    out = jnp.where(slot == 4, roll(vx, 3, 1), out)
    out = jnp.where(slot == 5, roll(vy, 4, 1), out)
    out = jnp.where(slot == 6, roll(vz, 5, 1), out)
    out = jnp.where(slot == 7, roll(ve, 6, 1), out)
    up[...] = out
    down[0] = jnp.where(slot < 3, roll(vr, -2, 1), jnp.where(slot < 6, roll(vi, 1, 1), roll(vx, 4, 1)))
    down[1] = jnp.where(slot < 2, roll(vy, -2, 1), jnp.where(slot < 4, vz, roll(ve, 2, 1)))


def tall(q, h, z):
    return jnp.concatenate([q[z], h[z]], axis=0)


def angles_at(trig, trig_halo, n, z):
    return jnp.concatenate([trig[n, z], trig_halo[n, z]], axis=0)


def advance(centre, above, below_turned, trig, edge, gain, lane):
    r, i = centre
    cz, sz, cx, sx, cy, sy = trig
    t = turned(cx, sx, ahead_x(r), ahead_x(i))
    w = turned_back(cx, sx, r, i)
    sum_r, sum_i = t[0] + behind_x(w[0]), t[1] + behind_x(w[1])
    if below_turned is not None:
        sum_r, sum_i = sum_r + below_turned[0], sum_i + below_turned[1]
    if above is not None:
        t = turned(cz, sz, *above)
        sum_r, sum_i = sum_r + t[0], sum_i + t[1]
    wr, wi = turned_back(cy, sy, r, i)
    fr, fi, wr, wi = roll(r, -1, 1), roll(i, -1, 1), roll(wr, 1, 1), roll(wi, 1, 1)
    if edge is not None:
        fr, fi = jnp.where(lane == 127, edge[0], fr), jnp.where(lane == 127, edge[1], fi)
        wr, wi = jnp.where(lane == 0, edge[0], wr), jnp.where(lane == 0, edge[1], wi)
    t = turned(cy, sy, fr, fi)
    sum_r, sum_i = sum_r + t[0] + wr, sum_i + t[1] + wi
    gain = gain - time_step * (r * r + i * i)
    return gain * r + time_step * sum_r, gain * i + time_step * sum_i


def begin(pr, pi, ep, trig, halo, trig_halo, br, bi):
    lane = iota((RX, LANES), 1)
    zero = jnp.zeros((RX, LANES), F32)

    def angles(z, carry):
        for n, k in enumerate((PZ, PX, PY)):
            trig_halo[2 * n, z], trig_halo[2 * n + 1, z] = sincos(halo[k, z])
        return carry

    lax.fori_loop(0, NZ, angles, 0)
    none = (zero, zero)

    def layer(z):
        return tall(pr, halo.at[PR], z), tall(pi, halo.at[PI], z)

    def one(z, above, below):
        t = [angles_at(trig, trig_halo, n, z) for n in range(6)]
        if below is not None:
            below = turned_back(angles_at(trig, trig_halo, 0, below), angles_at(trig, trig_halo, 1, below),
                                *layer(below))
        if above is not None:
            above = layer(above)
        br[z], bi[z] = advance(layer(z), above, below, t, none, tall(ep, halo.at[EP], z), lane)

    def body(z, carry):
        one(z, z + 1, z - 1)
        return carry

    lax.fori_loop(1, NZ - 1, body, 0)


def pack_edges(pr, pi, ep, trig, halo, own, lo, hi, strip, ntrig, part, strip_part, up, down):
    lane = iota((RX, LANES), 1)
    slot = lane % 8
    group = lane // 8
    gy = lax.axis_index("gy")
    keep = jnp.where((slot >= 2) & (slot < 5), jnp.where(gy < lax.axis_size("gy") - 1, 1, 0),
                     jnp.where((slot >= 5) & (slot < 7), jnp.where(gy > 0, 1, 0), 1)) > 0
    l = lo[...]
    a = hi[0]
    b = hi[1]
    zero = jnp.zeros_like(l)

    def join(k, from_hi, from_lo):
        v = own[k]
        out = jnp.where(slot < 2, v, roll(v, 5, 1))
        out = jnp.where((slot >= 2) & (slot < 5), from_hi, out)
        return jnp.where((slot == 5) | (slot == 6), from_lo, out)

    one = slot == 6
    strip[PR] = jnp.where(keep, join(PR, roll(a, 2, 1), roll(l, 5, 1)), zero)
    strip[PI] = jnp.where(keep, join(PI, roll(a, -1, 1), roll(l, 3, 1)), zero)
    strip[PX] = join(PX, roll(a, -4, 1), jnp.where(one, roll(l, 2, 1), zero))
    strip[PY] = join(PY, roll(b, 2, 1), jnp.where(one, roll(l, 1, 1), zero))
    strip[PZ] = join(PZ, b, jnp.where(one, l, zero))
    strip[EP] = join(EP, roll(b, -2, 1), jnp.where(one, roll(l, -1, 1), zero))
    for n, k in enumerate((PZ, PX, PY)):
        ntrig[2 * n], ntrig[2 * n + 1] = sincos(strip[k])
    keep_x, keep_xy = inside_masks()
    keep_tile = keep_x[NX:]
    sr, si = strip[PR], strip[PI]
    nt = [ntrig[n] for n in range(6)]
    w = turned_back(nt[0], nt[1], sr, si)
    below = [jnp.where(group > 0, roll(v, 8, 1), zero) for v in w]
    above = [jnp.where(group < NZ - 1, roll(v, -8, 1), zero) for v in (sr, si)]
    qr, qi = [jnp.where(keep_xy > 0, v, zero) for v in advance((sr, si), above, below, nt, None, strip[EP], lane)]
    strip_part[0] = qr
    strip_part[1] = qi
    er, ei = edge_columns(slot, ntrig, sr, si)

    def layer(z):
        return tall(pr, halo.at[PR], z), tall(pi, halo.at[PI], z)

    def angles_of(z):
        found = []
        for n, k in enumerate((PZ, PX, PY)):
            c, s = sincos(halo[k, z])
            found += [jnp.concatenate([trig[2 * n, z], c], axis=0), jnp.concatenate([trig[2 * n + 1, z], s], axis=0)]
        return found

    def first_step(z, above, below, t):
        edge = roll_by(er, shift_of(z)), roll_by(ei, shift_of(z))
        v = advance(layer(z), above, below, t, edge, tall(ep, halo.at[EP], z), lane)
        return masked_rows(v[0], keep_tile), masked_rows(v[1], keep_tile)

    def send(message, tiles, layers, strips):
        message[0], message[1] = tiles
        packed = strips[3]
        for k in range(3):
            packed = jnp.where(group == k, strips[k], packed)
        for k, v in enumerate((*layers, packed)):
            for t in range(RX // TILE):
                message[2 + 9 * k + t] = v[t * TILE:(t + 1) * TILE]

    low = first_step(0, layer(1), None, angles_of(0))
    t = angles_of(NZ - 1)
    c, s = sincos(halo[PZ, NZ - 2])
    below = turned_back(jnp.concatenate([trig[0, NZ - 2], c], axis=0), jnp.concatenate([trig[1, NZ - 2], s], axis=0),
                        *layer(NZ - 2))
    high = first_step(NZ - 1, None, below, t)
    part[0], part[1] = low
    part[2], part[3] = high
    turned_strips = (*w, *turned_back(nt[0], nt[1], qr, qi))
    send(up, turned_back(t[0][NX:], t[1][NX:], halo[PR, NZ - 1], halo[PI, NZ - 1]), turned_back(t[0], t[1], *high),
         [roll(v, 8 * (k - 15), 1) for k, v in enumerate(turned_strips)])
    send(down, (halo[PR, 0], halo[PI, 0]), low,
         [roll(v, 8 * k, 1) for k, v in enumerate((sr, si, qr, qi))])


def shift_of(group):
    return (125 - 8 * group) % 128


def on(test):
    return jnp.where(test, 1, 0)


def inside_masks():
    row = iota((RX, LANES), 0)
    slot = iota((RX, LANES), 1) % 8
    gx, gy = lax.axis_index("gx"), lax.axis_index("gy")
    keep_x = jnp.where(row < NX, 1, jnp.where(row < NX + 4, on(gx < lax.axis_size("gx") - 1), on(gx > 0)))
    keep_y = jnp.where((slot >= 2) & (slot < 5), on(gy < lax.axis_size("gy") - 1),
                       jnp.where((slot >= 5) & (slot < 7), on(gy > 0), 1))
    return keep_x, keep_x * keep_y


def edge_columns(slot, ntrig, r, i):
    wr, wi = turned_back(ntrig[4], ntrig[5], r, i)
    return jnp.where(slot == 3, roll(wr, -3, 1), r), jnp.where(slot == 3, roll(wi, -3, 1), i)


def masked_rows(v, keep_tile):
    return jnp.concatenate([v[:NX], jnp.where(keep_tile > 0, v[NX:], 0.0)], axis=0)


def analyse(z, r, i, trig_x, trig_y, columns, jx_column, lane, rows, out, spot):
    shift = shift_of(z)
    own_r, own_i = r[:NX], i[:NX]
    t = turned(trig_x[0][:NX], trig_x[1][:NX], ahead_x(r)[:NX], ahead_x(i)[:NX])
    jx = own_r * t[1] - own_i * t[0]
    last = lane == 127
    fr = jnp.where(last, roll_by(columns[0], shift), roll(r, -1, 1))
    fi = jnp.where(last, roll_by(columns[1], shift), roll(i, -1, 1))
    t = turned(*trig_y, fr, fi)
    jy = r * t[1] - i * t[0]
    jx_next = jnp.where(last[:NX], roll_by(jx_column[:NX], shift), roll(jx, -1, 1))
    circulation = jx + ahead_x(jy)[:NX] - jx_next - jy[:NX]
    rows[pl.ds(spot * NX, NX), :] = jx
    for j in range(NX // TILE):
        away = (j + out.shape[0] - lax.axis_index("gy")) % out.shape[0]
        out[away, spot] = circulation[j * TILE:(j + 1) * TILE]


def prefix(rows, out, spots, gap):
    triangle = triangle_of().astype(jnp.bfloat16)
    v = rows[spots.start * NX:spots.stop * NX, :]
    a = v.astype(jnp.bfloat16)
    v = v - a.astype(F32)
    b = v.astype(jnp.bfloat16)
    c = (v - b.astype(F32)).astype(jnp.bfloat16)
    sums = jnp.dot(jnp.concatenate([c, b, a], axis=0), triangle, preferred_element_type=F32)
    n = a.shape[0]
    sums = sums[:n] + sums[n:2 * n] + sums[2 * n:]
    for k, spot in enumerate(spots):
        for j in range(NX // TILE):
            away = (j + out.shape[0] - lax.axis_index("gy")) % out.shape[0]
            out[away, gap + spot] = sums[k * NX + j * TILE:k * NX + (j + 1) * TILE]


def roll_by(v, shift):
    return pltpu.roll(v, shift, 1)


def triangle_of():
    return jnp.where(iota((LANES, LANES), 0) <= iota((LANES, LANES), 1), 1.0, 0.0).astype(F32)


def interior(pr_in, pi_in, ep, trig, halo, trig_halo, strip, ntrig, part, strip_part, cr, ci, final_r, final_i, out,
             er, ei, nr, ni, jx_edge, rows):
    lane = iota((RX, LANES), 1)
    slot = lane % 8
    keep_x, keep_xy = inside_masks()
    keep_tile = keep_x[NX:]
    zero = jnp.zeros((RX, LANES), F32)
    nt = lambda: [ntrig[n] for n in range(6)]
    er[...], ei[...] = edge_columns(slot, ntrig, strip[PR], strip[PI])

    def fix(z, carry):
        shift = shift_of(z)
        xr, xi = roll_by(er[...], shift), roll_by(ei[...], shift)
        cy = jnp.where(lane == 127, angles_at(trig, trig_halo, 4, z), jnp.where(lane == 0, 1.0, 0.0)) * time_step
        sy = jnp.where(lane == 127, angles_at(trig, trig_halo, 5, z), 0.0) * time_step
        hr, hi = turned(cy, sy, xr, xi)
        cr[z] = masked_rows(pr_in[z] + hr, keep_tile)
        ci[z] = masked_rows(pi_in[z] + hi, keep_tile)
        return carry

    for z in range(1, NZ - 1):
        fix(z, 0)
    cr[0], ci[0], cr[NZ - 1], ci[NZ - 1] = part[0], part[1], part[2], part[3]

    def strips(r, i):
        w = turned_back(ntrig[0], ntrig[1], r, i)
        v = advance((r, i), (roll(r, -8, 1), roll(i, -8, 1)), (roll(w[0], 8, 1), roll(w[1], 8, 1)), nt(), None,
                    strip[EP], lane)
        return jnp.where(keep_xy > 0, v[0], zero), jnp.where(keep_xy > 0, v[1], zero)

    mr, mi = strip_part[0], strip_part[1]
    er[...], ei[...] = edge_columns(slot, ntrig, mr, mi)
    r, i = strips(mr, mi)
    nr[...] = r
    ni[...] = i
    t = turned(ntrig[2], ntrig[3], ahead_x(r), ahead_x(i))
    jx_edge[...] = r * t[1] - i * t[0]

    def second(z, carry):
        last_layer(z, (cr[z], ci[z]), (cr[z + 1], ci[z + 1]), (cr[z - 1], ci[z - 1]), ep, trig, halo, trig_halo,
                   (er[...], ei[...]), (nr[...], ni[...]), jx_edge[...], keep_x, lane, rows,
                   final_r, final_i, out, None, z - 2)
        return carry

    for z in range(2, NZ - 2):
        second(z, 0)
        if z % 4 == 1:
            prefix(rows, out, range(z - 5, z - 1), NZ - 4)


def last_layer(z, centre, above, below, ep, trig, halo, trig_halo, edges, columns, jx_column, keep_x, lane,
               rows, final_r, final_i, out, below_turned, spot):
    t = [angles_at(trig, trig_halo, n, z) for n in range(6)]
    if below_turned is None:
        below_turned = turned_back(angles_at(trig, trig_halo, 0, z - 1), angles_at(trig, trig_halo, 1, z - 1), *below)
    shift = shift_of(z)
    edge = roll_by(edges[0], shift), roll_by(edges[1], shift)
    r, i = advance(centre, above, below_turned, t, edge, tall(ep, halo.at[EP], z), lane)
    r = masked_rows(r, keep_x[NX:])
    i = masked_rows(i, keep_x[NX:])
    final_r[spot] = r[:NX]
    final_i[spot] = i[:NX]
    analyse(z, r, i, t[2:4], t[4:6], columns, jx_column, lane, rows, out, spot)


def boundary(pr, pi, ep, trig, halo, trig_halo, strip, ntrig, strip_part, cr, ci, middle_out,
             zlo, zhi, elo, ehi, final_r, final_i, out, rows):
    lane = iota((RX, LANES), 1)
    slot = lane % 8
    group = lane // 8
    keep_x, keep_xy = inside_masks()
    gz = lax.axis_index("gz")
    ok_hi = jnp.broadcast_to(on(gz < lax.axis_size("gz") - 1), (RX, LANES)) > 0
    ok_lo = jnp.broadcast_to(on(gz > 0), (RX, LANES)) > 0
    zero = jnp.zeros((RX, LANES), F32)
    for away in range(out.shape[0]):
        out[away, 8:] = middle_out[away]

    def piece(message, k):
        return jnp.concatenate([message[2 + 9 * k + t] for t in range(RX // TILE)], axis=0)

    def added(v, w):
        return tuple(a + time_step * b for a, b in zip(v, w))

    def masked(ok, v):
        return tuple(jnp.where(ok, u, zero) for u in v)

    lo_strip, hi_strip = piece(elo, 2), piece(ehi, 2)
    own = strip[PR], strip[PI]
    nt = [ntrig[n] for n in range(6)]
    from_lo = [roll(lo_strip, -8 * k, 1) for k in range(4)]
    from_hi = [roll(hi_strip, 8 * (15 - k), 1) for k in range(4)]
    at_lo, at_hi = ok_lo & (group == 0), ok_hi & (group == NZ - 1)
    beyond = turned(nt[0], nt[1], *from_hi[:2])
    middle = added((strip_part[0], strip_part[1]),
                   [jnp.where(at_lo, a, jnp.where(at_hi, b, zero)) for a, b in zip(from_lo, beyond)])
    lower = masked(ok_lo, added(from_lo[2:], own))
    upper = masked(ok_hi, added(from_hi[2:], turned_back(nt[0], nt[1], *own)))
    w = turned_back(nt[0], nt[1], *middle)
    below = [jnp.where(group == 0, a, roll(b, 8, 1)) for a, b in zip(lower, w)]
    above = [jnp.where(group == NZ - 1, a, roll(b, -8, 1)) for a, b in zip(upper, middle)]
    columns = masked(keep_xy > 0, advance(middle, above, below, nt, None, strip[EP], lane))
    edges = edge_columns(slot, ntrig, *middle)
    t = turned(nt[2], nt[3], ahead_x(columns[0]), ahead_x(columns[1]))
    jx_column = columns[0] * t[1] - columns[1] * t[0]

    def layer(z):
        return tall(pr, halo.at[PR], z), tall(pi, halo.at[PI], z)

    def got(main, tiles):
        return tuple(jnp.concatenate([main[n], tiles[n]], axis=0) for n in range(2))

    common = (ep, trig, halo, trig_halo, edges, columns, jx_column, keep_x, lane, rows, final_r, final_i, out)
    first = added((cr[0], ci[0]), masked(ok_lo, got(zlo, elo)))
    below = masked(ok_lo, added((piece(elo, 0), piece(elo, 1)), layer(0)))
    last_layer(0, first, (cr[1], ci[1]), None, *common, below, 0)
    last_layer(1, (cr[1], ci[1]), (cr[2], ci[2]), first, *common, None, 1)
    c, s = angles_at(trig, trig_halo, 0, NZ - 1), angles_at(trig, trig_halo, 1, NZ - 1)
    final = added((cr[15], ci[15]), turned(c, s, *masked(ok_hi, got(zhi, ehi))))
    above = masked(ok_hi, added((piece(ehi, 0), piece(ehi, 1)), turned_back(c, s, *layer(NZ - 1))))
    last_layer(14, (cr[14], ci[14]), final, (cr[13], ci[13]), *common, None, 2)
    last_layer(15, final, above, (cr[14], ci[14]), *common, None, 3)
    prefix(rows, out, range(4), 4)


def store(some_r, some_i, ends_r, ends_i, final_r, final_i, sems):
    pairs = []
    for some, ends, final in ((some_r, ends_r, final_r), (some_i, ends_i, final_i)):
        pairs += [(some, final.at[pl.ds(2, NZ - 4)]), (ends.at[pl.ds(0, 2)], final.at[pl.ds(0, 2)]),
                  (ends.at[pl.ds(2, 2)], final.at[pl.ds(NZ - 2, 2)])]
    for copy in start_copies(pairs, sems):
        copy.wait()


ENDS = (0, 1, NZ - 2, NZ - 1)


def finish(*refs):
    parts = lax.axis_size("gy")
    got, (circulation, flux, ends, middle, full_c, full_f, sems) = refs[:-7], refs[-7:]
    me = lax.axis_index("gy")
    for k in range(parts):
        source = (me + parts - k) % parts
        if k in EARLY:
            ends[source] = got[len(EARLY) + k][...]
            middle[source] = got[EARLY.index(k)][...]
        else:
            ends[source] = got[len(EARLY) + k][:8]
            middle[source] = got[len(EARLY) + k][8:]

    def layer(pieces, spot, gap, z):
        before = jnp.zeros((TILE, 1), F32)
        for j in range(parts):
            full_c[z, :, j * LANES:(j + 1) * LANES] = pieces[j, spot]
            v = pieces[j, spot + gap]
            full_f[z, :, j * LANES:(j + 1) * LANES] = v + before
            before = before + v[:, LANES - 1:]

    copies = []

    def send(first):
        for a, b in ((full_c, circulation), (full_f, flux)):
            copies.append(pltpu.make_async_copy(a.at[pl.ds(first, 4)], b.at[pl.ds(first, 4)], sems.at[len(copies)]))
            copies[-1].start()

    for first in (4, 8, 0, 12):
        for z in range(first, first + 4):
            if z in ENDS:
                layer(ends, ENDS.index(z), 4, z)
            else:
                layer(middle, z - 2, NZ - 4, z)
        send(first)
    for copy in copies:
        copy.wait()


def spec(*shape):
    return jax.ShapeDtypeStruct(shape, F32)


def call(body, outs, *args, scratch=(), hbm=0, smem=0, hbm_out=False):
    memory = [pl.BlockSpec(memory_space=pltpu.HBM if k < hbm else pltpu.SMEM if k < smem else pltpu.VMEM)
              for k in range(len(args))]
    return pl.pallas_call(
        body, out_shape=outs, in_specs=memory, scratch_shapes=list(scratch),
        out_specs=jax.tree.map(lambda _: pl.BlockSpec(memory_space=pltpu.HBM if hbm_out else pltpu.VMEM), outs),
        compiler_params=pltpu.CompilerParams(vmem_limit_bytes=32 * 2**20),
    )(*args)


def exchange(up, down, axis):
    size = lax.axis_size(axis)
    forward = [(k, (k + 1) % size) for k in range(size)]
    lo = lax.ppermute(up, axis, forward)
    hi = lax.ppermute(down, axis, [(b, a) for a, b in forward])
    return lo, hi


def ahead(value, k):
    size = lax.axis_size("gy")
    return lax.ppermute(value, "gy", [(i, (i + k) % size) for i in range(size)])


def program(pr_in, pi_in, pz_in, px_in, py_in, material, levels):
    parts = lax.axis_size("gy")
    pr, pi, px, py, pz = pr_in, pi_in, px_in, py_in, pz_in
    raw = (levels, pr, pi, px, py, pz, material)
    raw = tuple(pltpu.with_memory_space_constraint(a, pltpu.HBM) for a in raw)
    block, tall_block, strip_like = spec(NZ, NX, NY), spec(NZ, RX, LANES), spec(RX, LANES)
    scratch = lambda s, dtype=F32: pltpu.VMEM(s.shape, dtype)
    layers = spec(2, NX, NY)
    up, down, zup, zdown = call(pack_first, (spec(8, NZ, NY), spec(14, NZ, NY), layers, layers), *raw, hbm=7, scratch=[
        pltpu.SMEM((LEVELS,), F32), pltpu.VMEM((3, NZ, NY), F32), pltpu.VMEM((3, NZ, NY), jnp.int32),
        pltpu.VMEM((3, NX, NY), F32), pltpu.SemaphoreType.DMA((29,))])
    lo, hi = exchange(up, down, "gx")
    zlo, zhi = exchange(zup, zdown, "gz")
    own = call(columns, spec(6, NX, LANES), levels, pr, pi, px, py, pz, material, smem=1)
    halo, own, up, down = call(
        pack_y, (spec(6, NZ, TILE, LANES), spec(6, RX, LANES), strip_like, spec(2, RX, LANES)), own, lo, hi)
    lo, hi = exchange(up, down, "gy")
    ep, trig = call(angles, (block, spec(6, NZ, NX, NY)), levels, px, py, pz, material, smem=1)
    message = spec(2 + 3 * RX // TILE, TILE, LANES)
    strip, ntrig, part, strip_part, up, down = call(
        pack_edges, (spec(6, RX, LANES), spec(6, RX, LANES), spec(4, RX, LANES), spec(2, RX, LANES), message, message),
        pr, pi, ep, trig, halo, own, lo, hi)
    elo, ehi = exchange(up, down, "gz")
    trig_halo, br, bi = call(begin, (spec(6, NZ, TILE, LANES), tall_block, tall_block), pr, pi, ep, trig, halo)
    middle_block, ends_block = spec(NZ - 4, NX, NY), spec(4, NX, NY)
    cr, ci, some_r, some_i, out = call(
        interior, (tall_block, tall_block, middle_block, middle_block, spec(parts, 2 * NZ - 8, TILE, LANES)),
        br, bi, ep, trig, halo, trig_halo, strip, ntrig, part, strip_part,
        scratch=[scratch(strip_like)] * 5 + [pltpu.VMEM(((NZ - 4) * NX, NY), F32)])
    got = [ahead(out[k], k) for k in EARLY]
    ends_r, ends_i, out = call(
        boundary, (ends_block, ends_block, spec(parts, 2 * NZ, TILE, LANES)), pr, pi, ep, trig, halo, trig_halo, strip,
        ntrig, strip_part, cr, ci, out, zlo, zhi, elo, ehi, scratch=[pltpu.VMEM((4 * NX, NY), F32)])
    late = {k: ahead(out[k, :8] if k in EARLY else out[k], k) for k in LATE}
    final_r, final_i = call(store, (block, block), some_r, some_i, ends_r, ends_i, hbm_out=True,
                            scratch=[pltpu.SemaphoreType.DMA((6,))])
    got += [out[0]] + [late[k] for k in range(1, parts)]
    slab = spec(NZ, TILE, parts * LANES)
    circulation, flux = call(finish, (slab, slab), *got, hbm_out=True, scratch=[
        pltpu.VMEM((parts, 8, TILE, LANES), F32), pltpu.VMEM((parts, 2 * NZ - 8, TILE, LANES), F32),
        scratch(slab), scratch(slab), pltpu.SemaphoreType.DMA((8,))])
    return final_r, final_i, circulation, flux


def solution(mesh):
    block = P("gz", "gx", "gy")
    slab = P("gz", ("gx", "gy"), None)
    return jax.shard_map(program, mesh=mesh, in_specs=(block,) * 6 + (P(),),
                         out_specs=(block, block, slab, slab), check_vma=False)
```
